512 devices in a mesh: grp: 16 (over z), dev: 32 (over x, y, core).
Axes of the slice: x: 4, y: 4, z: 16, core: 2. Of those that a mesh axis runs over, the one named last changes fastest.
Arguments:
- root_solution: bfloat16 [4096, 256], P(('grp', 'dev')), may hold values from -6 to 6
- sep_rhs: bfloat16 [65536, 256], P(('grp', 'dev')), may hold values from -6 to 6
- sep_update: bfloat16 [65536, 512], P(('grp', 'dev')), may hold values from -0.25 to 0.25
- sep_rows: int32 [16, 512], P('grp'), may hold values from 0 to 4095
- sep_inv_cols: bfloat16 [65536, 4096], P(('grp', 'dev')), may hold values from -0.375 to 0.375
- leaf_rhs: bfloat16 [524288, 256], P(('grp', 'dev')), may hold values from -6 to 6
- leaf_update: bfloat16 [524288, 256], P(('grp', 'dev')), may hold values from -0.375 to 0.375
- leaf_rows: int32 [512, 256], P(('grp', 'dev')), may hold values from 0 to 8191
- leaf_cols: int32 [512], P(('grp', 'dev')), may hold values from 512 to 1024, as said below
- leaf_inv: bfloat16 [524288, 1024], P(('grp', 'dev')), may hold values from -0.1875 to 0.1875
Outputs:
- sep_solution: bfloat16 [65536, 256], P(('grp', 'dev'))
- leaf_solution: bfloat16 [524288, 256], P(('grp', 'dev'))
The draws below stay inside these ranges and needn't reach their ends.
Inputs may be any that keep to these rules, and one draw needn't show every extreme that they name: `leaf_cols`: some front has exactly 1024 live columns and some exactly 512.
All inputs are finite; a program needn't handle non-finite values.
Results may differ from the reference program's by a relative error of at most 0.0056.
Values may be sent and summed in bfloat16 or wider, within the bound.
No kernel may reach another device: no remote copies, remote signals or barrier semaphores. Data moves between devices by JAX's collectives and lax.ppermute only.
A program may use at most 64 MiB of HBM per device.

```python
import jax
import jax.numpy as jnp
from jax import lax

NRHS = 256
ROOT = 4096
SEP = 4096
RS = 512
LEAF = 1024
RL = 256
GROUPS = 16
FRONTS = 32


def draw_leaf_cols(key, part):
    total = GROUPS * FRONTS
    first_key, second_key = jax.random.split(jax.random.fold_in(key, 11))
    counts = jax.random.randint(first_key, (total,), LEAF // 2, LEAF + 1)
    places = jax.random.permutation(second_key, total)
    counts = counts.at[places[0]].set(LEAF)
    counts = counts.at[places[1]].set(LEAF // 2)
    return counts.astype(jnp.int32)


def plant(values, rng, low, top_value):
    longest = values.shape.index(max(values.shape))
    spots = []
    for shift in (0, 1):
        where = [jax.random.randint(jax.random.fold_in(rng, axis), (), 0, length) for axis, length in enumerate(values.shape)]
        where[longest] = (where[longest] + shift) % values.shape[longest]
        spots.append(tuple(where))
    return values.at[spots[0]].set(low).at[spots[1]].set(top_value)


def spiked(array, key, source, target, shards_of, factor):
    owner, partner = [(jnp.arange(array.shape[axis_at]) // (array.shape[axis_at] // shards_of)).reshape([-1 if axis == axis_at else 1 for axis in range(array.ndim)]) for axis_at in (source, target)]
    chosen = jax.random.permutation(key, shards_of)[partner]
    strong = (owner == chosen) | (owner == (partner + shards_of // 2) % shards_of)
    return jnp.where(strong, factor * array, array)


def level_of(stream_key, shape, pieces, low, top_value):
    loudness = 1.0
    for position, blocks in pieces:
        heights = jax.random.uniform(jax.random.fold_in(jax.random.fold_in(stream_key, 6), position), (blocks,), jnp.float32, low / len(pieces), top_value / len(pieces))
        loudness = loudness * jnp.repeat(jnp.exp(heights), shape[position] // blocks).reshape((-1,) + (1,) * (len(shape) - 1 - position))
    return loudness


def scatter_about(rng, dims, deviation, bound, cuts=(), kind=jnp.bfloat16):
    values = jax.random.normal(rng, dims, jnp.float32) * deviation
    if len(cuts) > 0:
        values = level_of(rng, dims, cuts, -0.22, 0.18) * values
    return jnp.clip(values, min=-bound, max=bound).astype(kind)


def heavy_noise(key, shape, spread, limit, cuts, heavy, kind=jnp.bfloat16):
    array = spread * jax.random.normal(key, shape, jnp.float32)
    if cuts:
        array = array * level_of(key, shape, cuts, -0.22, 0.18)
    return jnp.clip(spiked(array, jax.random.fold_in(key, 3), *heavy), -limit, limit).astype(kind)


def setup_inputs(seed: int = 0) -> dict:
    arg_keys = jax.random.split(jax.random.key(seed), 11)
    return {
        "root_solution": scatter_about(arg_keys[0], (ROOT, NRHS), 1.0, 6.0, ((0, 512),)),
        "sep_rhs": scatter_about(arg_keys[1], (GROUPS * SEP, NRHS), 1.0, 6.0, ((0, 512),)),
        "sep_update": scatter_about(arg_keys[2], (GROUPS * SEP, RS), RS ** -0.5, 0.25, ((0, 512),)),
        "sep_rows": plant(jax.random.randint(arg_keys[3], (GROUPS, RS), 0, ROOT), jax.random.fold_in(arg_keys[3], 1), 0, ROOT - 1).astype(jnp.int32),
        "sep_inv_cols": heavy_noise(arg_keys[4], (GROUPS * SEP, SEP), SEP ** -0.5, 0.375, ((0, 512),), (0, 1, 512, 6.0)),
        "leaf_rhs": scatter_about(arg_keys[5], (GROUPS * FRONTS * LEAF, NRHS), 1.0, 6.0, ((0, 512),)),
        "leaf_update": scatter_about(arg_keys[6], (GROUPS * FRONTS * LEAF, RL), RL ** -0.5, 0.375, ((0, 512),)),
        "leaf_rows": plant(jax.random.randint(arg_keys[7], (GROUPS * FRONTS, RL), 0, SEP + ROOT), jax.random.fold_in(arg_keys[7], 1), 0, (SEP + ROOT) - 1).astype(jnp.int32),
        "leaf_cols": draw_leaf_cols(jax.random.fold_in(arg_keys[10], 71), 0),
        "leaf_inv": scatter_about(arg_keys[9], (GROUPS * FRONTS * LEAF, LEAF), LEAF ** -0.5, 0.1875, ((0, 512),)),
    }


def reference(root_solution, sep_rhs, sep_update, sep_rows, sep_inv_cols, leaf_rhs, leaf_update, leaf_rows, leaf_cols, leaf_inv):
    def one_group(inputs):
        right_side, update, indices, inverse = inputs
        picked = jnp.take(root_solution, indices, axis=0)
        residual = (right_side.astype(jnp.float32) - jnp.dot(update, picked, preferred_element_type=jnp.float32)).astype(jnp.bfloat16)
        return jnp.dot(inverse.T, residual, preferred_element_type=jnp.float32).astype(jnp.bfloat16)

    sep_blocks = lax.map(one_group, (sep_rhs.reshape(GROUPS, SEP, NRHS), sep_update.reshape(GROUPS, SEP, RS), sep_rows, sep_inv_cols.reshape(GROUPS, SEP, SEP)))

    def one_leaf(inputs):
        group, right_side, update, indices, columns, inverse = inputs
        own_sep = lax.dynamic_index_in_dim(sep_blocks, group, 0, keepdims=False)
        ancestors = jnp.concatenate([own_sep, root_solution], axis=0)
        picked = jnp.take(ancestors, indices, axis=0)
        live_rows = (jnp.arange(LEAF, dtype=jnp.int32) < columns)[:, None]
        residual = right_side.astype(jnp.float32) - jnp.dot(update, picked, preferred_element_type=jnp.float32)
        residual = jnp.where(live_rows, residual, jnp.float32(0.0)).astype(jnp.bfloat16)
        solved = jnp.dot(inverse, residual, preferred_element_type=jnp.float32)
        return jnp.where(live_rows, solved, jnp.float32(0.0)).astype(jnp.bfloat16)

    group_ids = (jnp.arange(GROUPS * FRONTS, dtype=jnp.int32) // FRONTS).astype(jnp.int32)
    leaf_blocks = lax.map(one_leaf, (group_ids, leaf_rhs.reshape(GROUPS * FRONTS, LEAF, NRHS), leaf_update.reshape(GROUPS * FRONTS, LEAF, RL), leaf_rows, leaf_cols, leaf_inv.reshape(GROUPS * FRONTS, LEAF, LEAF)))
    return sep_blocks.reshape(GROUPS * SEP, NRHS), leaf_blocks.reshape(GROUPS * FRONTS * LEAF, NRHS)
```

```python
import jax
import jax.numpy as jnp
from jax import lax
from jax.experimental import pallas as pl
from jax.experimental.pallas import tpu as pltpu
from jax.sharding import Mesh
from jax.sharding import PartitionSpec as P

ALL = ("grp", "dev_0", "dev_1", "dev_2")
XY = ("dev_0", "dev_1")
CORE = "dev_2"
BF16, F32, I32 = jnp.bfloat16, jnp.float32, jnp.int32
MIB = 1 << 20


def to_all(blocks, axes):
    return lax.all_to_all(blocks, axes, 0, 0, tiled=True)


def swapped(value):
    return lax.ppermute(value, CORE, [(0, 1), (1, 0)])


def dot(a, b, dims=((1,), (0,))):
    return lax.dot_general(a, b, (dims, ((), ())), preferred_element_type=F32)


def picked(places, table):
    lines = lax.broadcasted_iota(I32, (places.shape[0], table.shape[0]), 1)
    chosen = jnp.where(lines == places, F32(1.0), F32(0.0)).astype(BF16)
    return dot(chosen, table)


def kernel_call(body, outs, flops, n_bytes, name, in_smem=()):
    def call(*args):
        specs = [
            pl.BlockSpec(memory_space=pltpu.SMEM if i in in_smem else pltpu.VMEM)
            for i in range(len(args))
        ]
        return pl.pallas_call(
            body,
            out_shape=outs,
            in_specs=specs,
            out_specs=jax.tree.map(lambda _: pl.BlockSpec(memory_space=pltpu.VMEM), outs),
            cost_estimate=pl.CostEstimate(flops=flops, bytes_accessed=n_bytes, transcendentals=0),
            compiler_params=pltpu.CompilerParams(vmem_limit_bytes=24 * MIB),
            name=name,
        )(*args)

    return call


def pick_body(places, table, out):
    out[...] = picked(places[...], table[...]).astype(BF16)


def residual_body(half, other, rhs, update, out):
    rows = half[...] + other[...]
    value = (rhs[...].astype(F32) - dot(update[...], rows)).astype(BF16)
    for i in range(out.shape[0]):
        out[i] = value


def partial_body(core, inverse, residual, own, other):
    both = dot(inverse[...], residual[...], ((0,), (0,)))
    half = both.shape[0] // 2
    low, high = both[:half], both[half:]
    first = core[0] == 0
    own[...] = jnp.where(first, low, high)
    other[...] = jnp.where(first, high, low)


def solution_body(own, other, out, copies):
    value = (own[...] + other[...]).astype(BF16)
    out[...] = value
    for i in range(copies.shape[0]):
        copies[i] = value


def ancestors_body(places, table, from_root, own, other):
    both = (picked(places[...], table[...]) + from_root[...].astype(F32)).astype(BF16)
    half = both.shape[0] // 2
    own[...] = both[:half]
    other[...] = both[half:]


def leaf_body(cols, own, other, rhs, update, inverse, out):
    rows = own[...] + other[...]
    live = lax.broadcasted_iota(I32, out.shape, 0) < cols[0]
    residual = rhs[...].astype(F32) - dot(update[...], rows)
    residual = jnp.where(live, residual, F32(0.0)).astype(BF16)
    solved = dot(inverse[...], residual)
    out[...] = jnp.where(live, solved, F32(0.0)).astype(BF16)


def on_device(
    root_solution,
    sep_rhs,
    sep_update,
    sep_rows,
    sep_inv_cols,
    leaf_rhs,
    leaf_update,
    leaf_rows,
    leaf_cols,
    leaf_inv,
):
    groups = lax.axis_size("grp")
    chips = lax.axis_size(XY)
    cores = lax.axis_size(CORE)
    devices = chips * cores
    core = lax.axis_index(CORE)
    own_root, nrhs = root_solution.shape
    own_sep, sep = sep_inv_cols.shape
    root = own_root * groups * devices
    held = sep // cores
    held_root = root // cores
    n_rows = leaf_rows.shape[1]

    def root_places(rows):
        device = rows // own_root % devices
        place = (device // cores * groups + rows // (own_root * devices)) * own_root + rows % own_root
        return jnp.where(device % cores == core, place, -1)

    def sep_places(rows):
        device = rows // own_sep
        return jnp.where(device % cores == core, device // cores * own_sep + rows % own_sep, -1)

    from_groups = to_all(jnp.broadcast_to(root_solution, (groups, own_root, nrhs)), "grp")
    own_lines = from_groups.reshape(groups * own_root, nrhs)
    root_held = to_all(jnp.broadcast_to(own_lines, (chips, *own_lines.shape)), XY)
    root_held = root_held.reshape(held_root, nrhs)

    blocks = sep_inv_cols.reshape(own_sep, chips, sep // chips).transpose(1, 0, 2)
    inverse = to_all(blocks, XY).reshape(held, sep // chips)

    both_rows = jnp.concatenate([leaf_rows[0], swapped(leaf_rows)[0]])
    at_root = jnp.where(both_rows >= sep, root_places(both_rows - sep), -1)[:, None]
    at_sep = jnp.where(both_rows < sep, sep_places(both_rows), -1)[:, None]

    rows_shape = jax.ShapeDtypeStruct((sep_rows.shape[1], nrhs), BF16)
    half = kernel_call(pick_body, rows_shape, 2 * rows_shape.size * held_root, 2 * MIB, "pick_sep")(
        root_places(sep_rows[0])[:, None], root_held
    )
    leaf_root = kernel_call(
        pick_body,
        jax.ShapeDtypeStruct((2 * n_rows, nrhs), BF16),
        4 * n_rows * nrhs * held_root,
        2 * MIB,
        "pick_leaf",
    )(at_root, root_held)

    copies_shape = jax.ShapeDtypeStruct((chips, own_sep, nrhs), BF16)
    part_shape = jax.ShapeDtypeStruct((own_sep, nrhs), F32)
    residual = kernel_call(residual_body, copies_shape, 2 * sep_update.size * nrhs, 2 * MIB, "residual")(
        half, swapped(half), sep_rhs, sep_update
    )
    residual = to_all(residual, XY).reshape(held, nrhs)
    own, other = kernel_call(
        partial_body, (part_shape, part_shape), 2 * inverse.size * nrhs, 3 * MIB, "partial", (0,)
    )(core.astype(I32)[None], inverse, residual)
    sep_out, copies = kernel_call(
        solution_body,
        (jax.ShapeDtypeStruct((own_sep, nrhs), BF16), copies_shape),
        part_shape.size,
        2 * MIB,
        "sum",
    )(own, swapped(other))
    sep_held = to_all(copies, XY).reshape(held, nrhs)

    half_shape = jax.ShapeDtypeStruct((n_rows, nrhs), BF16)
    own_rows, other_rows = kernel_call(
        ancestors_body, (half_shape, half_shape), 4 * n_rows * nrhs * held, 2 * MIB, "ancestors"
    )(at_sep, sep_held, leaf_root)
    leaf_out = kernel_call(
        leaf_body,
        jax.ShapeDtypeStruct(leaf_rhs.shape, BF16),
        2 * nrhs * (leaf_inv.size + leaf_update.size),
        4 * MIB,
        "leaf",
        (0,),
    )(leaf_cols, own_rows, swapped(other_rows), leaf_rhs, leaf_update, leaf_inv)
    return (sep_out, leaf_out)


def solution(mesh):
    finer = Mesh(mesh.devices.reshape(mesh.shape["grp"], 4, 4, 2), ALL)
    split = P(ALL, None)
    in_specs = (split, split, split, P("grp", None), split, split, split, split, P(ALL), split)
    return jax.shard_map(
        on_device, mesh=finer, in_specs=in_specs, out_specs=(split, split), check_vma=False
    )
```

```python
import functools

import jax
import jax.numpy as jnp
from jax import lax
from jax.experimental import pallas as pl
from jax.experimental.pallas import tpu as pltpu
from jax.sharding import Mesh
from jax.sharding import PartitionSpec as P

ALL = ("grp", "dev_0", "dev_1", "dev_2")
XY = ("dev_0", "dev_1")
CORE = "dev_2"
BF16, F32, I32 = jnp.bfloat16, jnp.float32, jnp.int32
MIB = 1 << 20


def to_all(blocks, axes):
    return lax.all_to_all(blocks, axes, 0, 0, tiled=True)


def swapped(value):
    return lax.ppermute(value, CORE, [(0, 1), (1, 0)])


def dot(a, b, dims=((1,), (0,))):
    return lax.dot_general(a, b, (dims, ((), ())), preferred_element_type=F32)


def column(row):
    size = 128
    eye = lax.broadcasted_iota(I32, (size, size), 0) == lax.broadcasted_iota(I32, (size, size), 1)
    parts = [
        jnp.sum(jnp.where(eye, row[:, i : i + size], F32(0.0)), axis=1, keepdims=True)
        for i in range(0, row.shape[1], size)
    ]
    return jnp.concatenate(parts, axis=0)


def chosen(places, lines):
    if places.shape[0] == 1:
        places = column(places.astype(F32)).astype(I32)
    at = lax.broadcasted_iota(I32, (places.shape[0], lines), 1)
    return jnp.where(at == places, F32(1.0), F32(0.0)).astype(BF16)


def kernel_call(body, outs, flops, n_bytes, in_smem=(), limit=16, in_hbm=(), scratch=()):
    def call(*args):
        specs = [
            pl.BlockSpec(
                memory_space=pltpu.SMEM if i in in_smem else pltpu.HBM if i in in_hbm else pltpu.VMEM
            )
            for i in range(len(args))
        ]
        return pl.pallas_call(
            body,
            out_shape=outs,
            in_specs=specs,
            out_specs=jax.tree.map(lambda _: pl.BlockSpec(memory_space=pltpu.VMEM), outs),
            scratch_shapes=scratch,
            cost_estimate=pl.CostEstimate(flops=flops, bytes_accessed=n_bytes, transcendentals=0),
            compiler_params=pltpu.CompilerParams(vmem_limit_bytes=int(limit * MIB)),
        )(*args)

    return call


def log2(size):
    assert size & (size - 1) == 0
    return size.bit_length() - 1


def root_places(rows, own, cores, devices, groups):
    line = rows & (own - 1)
    device = (rows >> log2(own)) & (devices - 1)
    group = rows >> log2(own * devices)
    chip, core = device >> log2(cores), device & (cores - 1)
    return (((chip << log2(groups)) + group << log2(cores)) + core << log2(own)) + line


def side(first, value):
    half = value.shape[1] // 2
    return jnp.where(first, value[:, :half], value[:, half:])


def joined(first, mine, theirs):
    return jnp.concatenate(
        [jnp.where(first, mine, theirs), jnp.where(first, theirs, mine)], axis=1
    )


def pack_body(core, rhs, update, out):
    half = rhs.shape[1] // 2
    out[:, :half] = side(core[0] != 0, rhs[...])
    out[:, half:] = update[...]


def spread_body(sizes, core, rows, rhs, update, arrived, rhs_out, spread_out):
    half = rhs.shape[1] // 2
    rhs_out[...] = jnp.concatenate([side(core[0] == 0, rhs[...]), arrived[:, :half]], axis=0)
    both = jnp.concatenate([update[...], arrived[:, half:]], axis=0)
    at = chosen(root_places(rows[...], *sizes), spread_out.shape[1])
    spread_out[...] = dot(both, at).astype(BF16)


def terms_body(rhs, spread, table, own_inverse_at, other_inverse_at, out, own_inverse, other_inverse, sems):
    copies = (
        pltpu.make_async_copy(own_inverse_at, own_inverse, sems.at[0]),
        pltpu.make_async_copy(other_inverse_at, other_inverse, sems.at[1]),
    )
    for copy in copies:
        copy.start()
    residual = rhs[...].astype(F32) - dot(spread[...], table[...])
    residual = residual.astype(BF16).astype(F32).T.astype(BF16)
    chips, _, wide = out.shape
    for copy in copies:
        copy.wait()
    for i in range(chips):
        at = slice(i * wide, (i + 1) * wide)
        both = jnp.concatenate([own_inverse[:, at], other_inverse[:, at]], axis=0)
        out[i] = dot(residual, both).astype(BF16)


def sum_body(terms, out, copies):
    total = terms[0].astype(F32)
    for i in range(1, terms.shape[0]):
        total = total + terms[i].astype(F32)
    value = total.T.astype(BF16)
    out[...] = value
    for i in range(copies.shape[0]):
        copies[i] = value


def leaf_root_body(sizes, sep, own_rows, other_rows, table, picked_out, at_out):
    rows = jnp.concatenate([own_rows[...], other_rows[...]], axis=1)
    at = jnp.where(rows >= sep, root_places(rows - sep, *sizes), -1)
    picked_out[...] = dot(chosen(at, table.shape[0]), table[...]).astype(BF16)
    at_out[...] = column(jnp.where(rows < sep, rows, -1).astype(F32)).astype(I32)


def sep_out_body(core, value, arrived, out):
    rows = out.shape[0]
    both = value[...]
    out[...] = joined(
        core[0] == 0, jnp.where(core[0] == 0, both[:rows], both[rows:]), arrived[...]
    )


def ancestors_body(at, table, from_root, own, other):
    rows = dot(chosen(at[...], table.shape[0]), table[...])
    rows = (rows + from_root[...].astype(F32)).astype(BF16)
    half = rows.shape[0] // 2
    own[...] = rows[:half]
    other[...] = rows[half:]


def leaf_body(core, cols, own, other, rhs_at, update_at, inverse_at, out, rhs, update, inverse, sems):
    fetches = [
        pltpu.make_async_copy(source, target, sems.at[i])
        for i, (source, target) in enumerate(
            ((update_at, update), (rhs_at, rhs), (inverse_at, inverse))
        )
    ]
    for fetch in fetches:
        fetch.start()
    rows = joined(core[0] == 0, own[...], other[...])
    live = lax.broadcasted_iota(I32, out.shape, 0) < cols[0]
    fetches[0].wait()
    value = dot(update[...], rows)
    fetches[1].wait()
    residual = jnp.where(live, rhs[...].astype(F32) - value, F32(0.0)).astype(BF16)
    fetches[2].wait()
    solved = dot(inverse[...], residual)
    out[...] = jnp.where(live, solved, F32(0.0)).astype(BF16)


def on_device(
    root_solution,
    sep_rhs,
    sep_update,
    sep_rows,
    sep_inv_cols,
    leaf_rhs,
    leaf_update,
    leaf_rows,
    leaf_cols,
    leaf_inv,
):
    groups = lax.axis_size("grp")
    chips = lax.axis_size(XY)
    cores = lax.axis_size(CORE)
    devices = chips * cores
    core = lax.axis_index(CORE).astype(I32)[None]
    own_root, nrhs = root_solution.shape
    own_sep, sep = sep_inv_cols.shape
    root = own_root * groups * devices
    wide = nrhs // cores
    n_sep, n_leaf = sep_rows.shape[1], leaf_rows.shape[1]
    n_both = cores * own_sep
    sizes = (own_root, cores, devices, groups)

    def array(*shape, dtype=BF16):
        return jax.ShapeDtypeStruct(shape, dtype)

    blocks = root_solution.reshape(own_root, cores, wide).swapaxes(0, 1)
    blocks = jnp.broadcast_to(blocks, (groups, cores, own_root, wide))
    lines = to_all(blocks.reshape(groups * cores, own_root, wide), ("grp", CORE))
    lines = lines.reshape(groups * cores * own_root, wide)
    blocks = jnp.broadcast_to(lines, (chips, *lines.shape))
    root_all = to_all(blocks, XY).reshape(root, wide)

    other_inverse = swapped(sep_inv_cols)
    sent = kernel_call(
        pack_body, array(own_sep, wide + n_sep), own_sep, MIB, (0,), 4
    )(core, sep_rhs, sep_update)
    arrived = swapped(sent)
    other_rows = swapped(leaf_rows)

    rhs, spread = kernel_call(
        functools.partial(spread_body, sizes),
        (array(n_both, wide), array(n_both, root)),
        2 * n_both * n_sep * root,
        4 * MIB,
        (0,),
    )(core, sep_rows, sep_rhs, sep_update, arrived)

    terms = kernel_call(
        terms_body,
        array(chips, wide, sep // chips),
        2 * n_both * wide * (root + sep),
        6 * MIB,
        limit=16,
        in_hbm=(3, 4),
        scratch=(
            pltpu.VMEM(sep_inv_cols.shape, BF16),
            pltpu.VMEM(sep_inv_cols.shape, BF16),
            pltpu.SemaphoreType.DMA((2,)),
        ),
    )(rhs, spread, root_all, sep_inv_cols, other_inverse)
    terms = to_all(terms, XY)
    value, copies = kernel_call(
        sum_body, (array(n_both, wide), array(chips, n_both, wide)), terms.size, 2 * MIB
    )(terms)
    sep_all = to_all(copies, XY).reshape(sep, wide)

    theirs = lax.dynamic_slice_in_dim(value, (1 - core[0]) * own_sep, own_sep, 0)
    theirs = swapped(theirs)
    sep_out = kernel_call(
        sep_out_body, array(own_sep, nrhs), own_sep, MIB, (0,), 4
    )(core, value, theirs)

    leaf_root, at_leaf = kernel_call(
        functools.partial(leaf_root_body, sizes, sep),
        (array(cores * n_leaf, wide), array(cores * n_leaf, 1, dtype=I32)),
        2 * cores * n_leaf * wide * root,
        6 * MIB,
    )(leaf_rows, other_rows, root_all)
    own_rows, sent_rows = kernel_call(
        ancestors_body,
        (array(n_leaf, wide), array(n_leaf, wide)),
        2 * cores * n_leaf * wide * sep,
        6 * MIB,
    )(at_leaf, sep_all, leaf_root)
    arrived_rows = swapped(sent_rows)
    leaf_out = kernel_call(
        leaf_body,
        array(*leaf_rhs.shape),
        2 * nrhs * (leaf_inv.size + leaf_update.size),
        4 * MIB,
        (0, 1),
        limit=63.2,
        in_hbm=(4, 5, 6),
        scratch=(
            pltpu.VMEM(leaf_rhs.shape, BF16),
            pltpu.VMEM(leaf_update.shape, BF16),
            pltpu.VMEM(leaf_inv.shape, BF16),
            pltpu.SemaphoreType.DMA((3,)),
        ),
    )(core, leaf_cols, own_rows, arrived_rows, leaf_rhs, leaf_update, leaf_inv)
    return (sep_out, leaf_out)


def solution(mesh):
    finer = Mesh(mesh.devices.reshape(mesh.shape["grp"], 4, 4, 2), ALL)
    split = P(ALL, None)
    in_specs = (split, split, split, P("grp", None), split, split, split, split, P(ALL), split)
    return jax.shard_map(
        on_device, mesh=finer, in_specs=in_specs, out_specs=(split, split), check_vma=False
    )
```

```python
import functools

import jax
import jax.numpy as jnp
from jax import lax
from jax.experimental import pallas as pl
from jax.experimental.pallas import tpu as pltpu
from jax.sharding import Mesh
from jax.sharding import PartitionSpec as P

ALL = ("grp", "dev_0", "dev_1", "dev_2")
XY = ("dev_0", "dev_1")
SLOTS, LIST = 64, 8
BASE = 64
CORE = "dev_2"
BF16, F32, I32 = jnp.bfloat16, jnp.float32, jnp.int32
MIB = 1 << 20


def to_all(blocks, axes):
    return lax.all_to_all(blocks, axes, 0, 0, tiled=True)


def swapped(value):
    return lax.ppermute(value, CORE, [(0, 1), (1, 0)])


def dot(a, b, dims=((1,), (0,))):
    return lax.dot_general(a, b, (dims, ((), ())), preferred_element_type=F32)


def column(row):
    size = 128
    eye = lax.broadcasted_iota(I32, (size, size), 0) == lax.broadcasted_iota(I32, (size, size), 1)
    parts = [
        jnp.sum(jnp.where(eye, row[:, i : i + size], F32(0.0)), axis=1, keepdims=True)
        for i in range(0, row.shape[1], size)
    ]
    return jnp.concatenate(parts, axis=0)


def chosen(places, lines):
    if places.shape[0] == 1:
        places = column(places.astype(F32)).astype(I32)
    at = lax.broadcasted_iota(I32, (places.shape[0], lines), 1)
    return jnp.where(at == places, F32(1.0), F32(0.0)).astype(BF16)


def kernel_call(body, outs, flops, n_bytes, in_smem=(), limit=16, in_hbm=(), scratch=()):
    def call(*args):
        specs = [
            pl.BlockSpec(
                memory_space=pltpu.SMEM if i in in_smem else pltpu.HBM if i in in_hbm else pltpu.VMEM
            )
            for i in range(len(args))
        ]
        return pl.pallas_call(
            body,
            out_shape=outs,
            in_specs=specs,
            out_specs=jax.tree.map(
                lambda out: pl.BlockSpec(
                    memory_space=pltpu.SMEM if out.ndim == 1 else pltpu.VMEM
                ),
                outs,
            ),
            scratch_shapes=scratch,
            cost_estimate=pl.CostEstimate(
                flops=flops, bytes_accessed=n_bytes, transcendentals=0
            ),
            compiler_params=pltpu.CompilerParams(vmem_limit_bytes=int(limit * MIB)),
        )(*args)

    return call


def log2(size):
    assert size & (size - 1) == 0
    return size.bit_length() - 1


def root_owner(rows, own, cores, devices, groups):
    device = (rows >> log2(own)) & (devices - 1)
    line = ((rows >> log2(own * devices)) << log2(cores)) + (device & (cores - 1))
    return device >> log2(cores), (line << log2(own)) + (rows & (own - 1))


def ancestor_owner(sizes, sep, held, rows):
    chip, line = root_owner(rows - sep, *sizes)
    here = rows < sep
    return jnp.where(here, rows >> log2(held), chip), jnp.where(here, rows & (held - 1), held + line)


def before(size):
    lines = lax.broadcasted_iota(I32, (size, size), 0)
    return one(lines < lax.broadcasted_iota(I32, (size, size), 1))


def one(mask):
    return jnp.where(mask, F32(1.0), F32(0.0)).astype(BF16)


def encoded(rows):
    digits = [rows >> log2(BASE), rows & (BASE - 1)]
    size = 128
    lines = [d[:, i : i + size] for d in digits for i in range(0, rows.shape[1], size)]
    return jnp.concatenate(lines, axis=0).astype(F32).astype(BF16)


def decoded(lines):
    value = lines.astype(F32)
    half = value.shape[0] // 2
    value = value[:half] * F32(BASE) + value[half:]
    return jnp.concatenate([value[i : i + 1] for i in range(half)], axis=1).astype(I32)


def side(first, value):
    half = value.shape[1] // 2
    return jnp.where(first, value[:, :half], value[:, half:])


def of_core(first, value):
    half = value.shape[0] // 2
    return jnp.where(first, value[:half], value[half:])


def joined(first, mine, theirs):
    return jnp.concatenate(
        [jnp.where(first, mine, theirs), jnp.where(first, theirs, mine)], axis=1
    )


def fan_body(root, out):
    half = root.shape[1] // 2
    low, high = root[:, :half], root[:, half:]
    for i in range(0, out.shape[0], 2):
        out[i] = low
        out[i + 1] = high


def pack_body(core, rhs, update, leaf_rows, out):
    rows, half = rhs.shape[0], rhs.shape[1] // 2
    out[:rows, :half] = side(core[0] != 0, rhs[...])
    out[:rows, half:] = update[...]
    listed = leaf_rows[...]
    digits = jnp.concatenate([listed >> log2(BASE), listed & (BASE - 1)], axis=1)
    spare = out.shape[0] - rows
    digits = jnp.broadcast_to(digits.astype(F32), (spare, digits.shape[1]))
    out[rows:, : digits.shape[1]] = digits.astype(BF16)
    out[rows:, digits.shape[1] :] = jnp.zeros((spare, out.shape[1] - digits.shape[1]), BF16)


def plan_body(
    sizes, me, rows, rhs, update, leaf_rows, arrived, rhs_out, spread_out, select_out, list_out, fits_out
):
    own, half = rhs.shape[0], rhs.shape[1] // 2
    core, chip = me[0], me[1]
    rhs_out[...] = jnp.concatenate([side(core == 0, rhs[...]), arrived[:own, :half]], axis=0)
    both = jnp.concatenate([update[...], arrived[:own, half:]], axis=0)

    chips = spread_out.shape[1] // SLOTS
    wanted = rows[...]
    size = wanted.shape[1]
    owner, line = root_owner(wanted, *sizes)
    owned = lax.broadcasted_iota(I32, (chips, size), 0) == owner
    rank = jnp.where(owned, dot(one(owned), before(size)), F32(0.0))
    rank = jnp.sum(rank, axis=0, keepdims=True).astype(I32)
    most = jnp.max(rank.astype(F32))
    fits = (most < F32(SLOTS)).astype(I32)
    fits_out[0] = fits
    place = jnp.where(fits == 1, owner * SLOTS + rank, lax.broadcasted_iota(I32, (1, size), 1))
    spread_out[...] = dot(both, chosen(place, spread_out.shape[1])).astype(BF16)

    mine = jnp.where(owner == chip, rank, -1)
    slot = one(lax.broadcasted_iota(I32, (SLOTS, size), 0) == mine)
    lines = select_out.shape[1]
    source = one(lax.broadcasted_iota(I32, (lines, size), 0) == line)
    select_out[...] = dot(slot, source, ((1,), (1,))).astype(BF16)

    n_leaf = leaf_rows.shape[1]
    digits = arrived[own:, : 2 * n_leaf].astype(F32)[:1]
    other = (digits[:, :n_leaf] * F32(BASE) + digits[:, n_leaf:]).astype(I32)
    list_out[...] = encoded(jnp.concatenate([leaf_rows[...], other], axis=1))


def select_body(select, lines, listed, out):
    rows = dot(select[...], lines[...]).astype(BF16)
    listed = listed[...]
    for i in range(out.shape[0]):
        out[i, :SLOTS] = rows
        out[i, SLOTS:] = listed


def all_lines_body(lines, listed, out):
    held = lines.shape[0]
    for i in range(out.shape[0]):
        out[i, :held] = lines[...]
        out[i, held:] = listed[...]


def all_rows_body(sizes, rows, arrived, out):
    chips, held, wide = arrived.shape
    held = held - LIST
    owner, line = root_owner(rows[...], *sizes)
    table = arrived[:, :held].reshape(chips * held, wide)
    picked = dot(chosen(owner * held + line, chips * held), table).astype(BF16)
    full = picked.shape[0] // SLOTS
    out[:full, :SLOTS] = picked.reshape(full, SLOTS, wide)
    out[full:, :SLOTS] = jnp.zeros((chips - full, SLOTS, wide), BF16)
    out[:, SLOTS:] = arrived[:, held:]


def terms_body(rhs, spread, arrived, own_inverse_at, other_inverse_at, out, own_inverse, other_inverse, sems):
    copies = (
        pltpu.make_async_copy(own_inverse_at, own_inverse, sems.at[0]),
        pltpu.make_async_copy(other_inverse_at, other_inverse, sems.at[1]),
    )
    for copy in copies:
        copy.start()
    chips, _, width = out.shape
    wide = rhs.shape[1]
    table = arrived[:, :SLOTS].reshape(chips * SLOTS, wide)
    residual = rhs[...].astype(F32) - dot(spread[...], table)
    residual = residual.astype(BF16).astype(F32).T.astype(BF16)
    for copy in copies:
        copy.wait()
    for i in range(chips):
        at = slice(i * width, (i + 1) * width)
        both = jnp.concatenate([own_inverse[:, at], other_inverse[:, at]], axis=0)
        out[i] = dot(residual, both).astype(BF16)


def leaf_plan_body(sizes, sep, held, me, arrived, select_out, place_out, fits_out, mine_at, line_at):
    chips = arrived.shape[0]
    chip = me[1]
    rows = jnp.concatenate([decoded(arrived[i, SLOTS:]) for i in range(chips)], axis=0)
    size = rows.shape[1]
    owner, line = ancestor_owner(sizes, sep, held, rows)
    counts = before(size)
    owned = jnp.concatenate([owner == i for i in range(chips)], axis=0)
    rank = jnp.where(owned, dot(one(owned), counts), F32(0.0))
    fits = (jnp.max(rank) < F32(SLOTS)).astype(I32)
    fits_out[0] = fits

    listed = lax.broadcasted_iota(I32, (chips, 1), 0) == chip
    own_rank = jnp.zeros((1, size), F32)
    for i in range(chips):
        part = rank[i * chips : (i + 1) * chips]
        own_rank = own_rank + jnp.sum(jnp.where(listed, part, F32(0.0)), axis=0, keepdims=True)
    own_owner = jnp.sum(jnp.where(listed, owner.astype(F32), F32(0.0)), axis=0, keepdims=True)
    place = own_owner * F32(SLOTS) + own_rank
    place = jnp.where(fits == 1, place, lax.broadcasted_iota(I32, (1, size), 1).astype(F32))
    place_out[...] = column(place).astype(I32)

    mine = owner == chip
    mine_at[...] = jnp.where(mine, dot(one(mine), counts), F32(-1.0)).astype(I32)
    line_at[...] = line

    def step(i, _):
        slot = one(lax.broadcasted_iota(I32, (SLOTS, size), 0) == mine_at[pl.ds(i, 1), :])
        lines = select_out.shape[2]
        source = one(lax.broadcasted_iota(I32, (lines, size), 0) == line_at[pl.ds(i, 1), :])
        select_out[i] = dot(slot, source, ((1,), (1,))).astype(BF16)
        return 0

    lax.fori_loop(0, chips, step, 0)


def sum_body(terms, select, lines, out, blocks):
    total = terms[0].astype(F32)
    for i in range(1, terms.shape[0]):
        total = total + terms[i].astype(F32)
    value = total.T.astype(BF16)
    out[...] = value
    table = jnp.concatenate([value, lines[...]], axis=0)
    chips, slots, size = select.shape
    rows = dot(select[...].reshape(chips * slots, size), table).astype(BF16)
    blocks[...] = rows.reshape(blocks.shape)


def all_ancestors_body(sizes, sep, held, listed, arrived, out):
    chips, lines, wide = arrived.shape
    owner, line = ancestor_owner(sizes, sep, held, decoded(listed[...]))
    place = owner * lines + line
    total = jnp.zeros((place.shape[1], wide), F32)
    for i in range(chips):
        total = total + dot(chosen(place - i * lines, lines), arrived[i])
    full = total.shape[0] // SLOTS
    out[:full] = total.astype(BF16).reshape(full, SLOTS, wide)
    out[full:] = jnp.zeros((chips - full, SLOTS, wide), BF16)


def ancestors_body(me, place, arrived, value, own, sent):
    chips, slots, wide = arrived.shape
    table = arrived[...].reshape(chips * slots, wide)
    rows = dot(chosen(place[...], chips * slots), table).astype(BF16)
    half = rows.shape[0] // 2
    own[...] = rows[:half]
    sent[:half] = rows[half:]
    sent[half:] = of_core(me[0] != 0, value[...])


def leaf_body(
    me, cols, own, arrived, value, rhs_at, update_at, inverse_at, out, sep_out, rhs, update, inverse, sems
):
    fetches = [
        pltpu.make_async_copy(source, target, sems.at[i])
        for i, (source, target) in enumerate(
            ((update_at, update), (rhs_at, rhs), (inverse_at, inverse))
        )
    ]
    for fetch in fetches:
        fetch.start()
    first, half = me[0] == 0, own.shape[0]
    rows = joined(first, own[...], arrived[:half])
    sep_out[...] = joined(first, of_core(first, value[...]), arrived[half:])
    live = lax.broadcasted_iota(I32, out.shape, 0) < cols[0]
    fetches[0].wait()
    term = dot(update[...], rows)
    fetches[1].wait()
    residual = jnp.where(live, rhs[...].astype(F32) - term, F32(0.0)).astype(BF16)
    fetches[2].wait()
    solved = dot(inverse[...], residual)
    out[...] = jnp.where(live, solved, F32(0.0)).astype(BF16)


def on_device(
    root_solution,
    sep_rhs,
    sep_update,
    sep_rows,
    sep_inv_cols,
    leaf_rhs,
    leaf_update,
    leaf_rows,
    leaf_cols,
    leaf_inv,
):
    groups = lax.axis_size("grp")
    chips = lax.axis_size(XY)
    cores = lax.axis_size(CORE)
    devices = chips * cores
    me = jnp.stack([lax.axis_index(CORE), lax.axis_index(XY)]).astype(I32)
    own_root, nrhs = root_solution.shape
    own_sep, sep = sep_inv_cols.shape
    wide = nrhs // cores
    n_sep, n_leaf = sep_rows.shape[1], leaf_rows.shape[1]
    held = cores * own_sep
    lines_here = groups * cores * own_root
    sizes = (own_root, cores, devices, groups)

    def array(*shape, dtype=BF16):
        return jax.ShapeDtypeStruct(shape, dtype)

    flag = array(1, dtype=I32)

    blocks = kernel_call(fan_body, array(groups * cores, own_root, wide), 1024, MIB, limit=4)(
        root_solution
    )
    lines = to_all(blocks, ("grp", CORE)).reshape(lines_here, wide)

    other_inverse = swapped(sep_inv_cols)
    sent = kernel_call(
        pack_body, array(own_sep + 8, wide + n_sep), own_sep, MIB, (0,), 4
    )(me, sep_rhs, sep_update, leaf_rows)
    arrived = swapped(sent)

    rhs, spread, select, listed, fits = kernel_call(
        functools.partial(plan_body, sizes),
        (
            array(held, wide),
            array(held, chips * SLOTS),
            array(SLOTS, lines_here),
            array(LIST, 128),
            flag,
        ),
        2 * held * n_sep * chips * SLOTS,
        MIB,
        (0,),
    )(me, sep_rows, sep_rhs, sep_update, leaf_rows, arrived)

    mail = array(chips, SLOTS + LIST, wide)
    blocks = kernel_call(select_body, mail, SLOTS * lines_here * wide, MIB, limit=4)(
        select, lines, listed
    )

    def few_rows(blocks, lines, listed, sep_rows):
        return to_all(blocks, XY)

    def all_rows(blocks, lines, listed, sep_rows):
        full = array(chips, lines_here + LIST, wide)
        full = kernel_call(all_lines_body, full, 1024, 2 * MIB)(lines, listed)
        return kernel_call(functools.partial(all_rows_body, sizes), mail, 1024, 2 * MIB)(sep_rows, to_all(full, XY))

    root_rows = lax.cond(fits[0] == 1, few_rows, all_rows, blocks, lines, listed, sep_rows)

    terms = kernel_call(
        terms_body,
        array(chips, wide, sep // chips),
        2 * held * wide * (chips * SLOTS + sep),
        6 * MIB,
        in_hbm=(3, 4),
        scratch=(
            pltpu.VMEM(sep_inv_cols.shape, BF16),
            pltpu.VMEM(sep_inv_cols.shape, BF16),
            pltpu.SemaphoreType.DMA((2,)),
        ),
    )(rhs, spread, root_rows, sep_inv_cols, other_inverse)
    terms = to_all(terms, XY)

    select, place, fits = kernel_call(
        functools.partial(leaf_plan_body, sizes, sep, held),
        (
            array(chips, SLOTS, held + lines_here),
            array(cores * n_leaf, 1, dtype=I32),
            flag,
        ),
        chips * 2**26,
        2 * MIB,
        (0,),
        scratch=(
            pltpu.VMEM((chips, cores * n_leaf), I32),
            pltpu.VMEM((chips, cores * n_leaf), I32),
        ),
    )(me, root_rows)
    mail = array(chips, SLOTS, wide)
    value, blocks = kernel_call(
        sum_body, (array(held, wide), mail), 2 * chips * SLOTS * wide * (held + lines_here), 2 * MIB
    )(terms, select, lines)

    def few_ancestors(blocks, value, lines, listed):
        return to_all(blocks, XY)

    def all_ancestors(blocks, value, lines, listed):
        table = jnp.concatenate([value, lines], axis=0)
        table = to_all(jnp.broadcast_to(table, (chips, *table.shape)), XY)
        return kernel_call(functools.partial(all_ancestors_body, sizes, sep, held), mail, 1024, 2 * MIB)(listed, table)

    ancestors = lax.cond(fits[0] == 1, few_ancestors, all_ancestors, blocks, value, lines, listed)

    own_rows, sent = kernel_call(
        ancestors_body,
        (array(n_leaf, wide), array(n_leaf + own_sep, wide)),
        2 * cores * n_leaf * wide * chips * SLOTS,
        MIB,
        (0,),
    )(me, place, ancestors, value)
    arrived = swapped(sent)
    leaf_out, sep_out = kernel_call(
        leaf_body,
        (array(*leaf_rhs.shape), array(own_sep, nrhs)),
        2 * nrhs * (leaf_inv.size + leaf_update.size),
        4 * MIB,
        (0, 1),
        limit=62.8,
        in_hbm=(5, 6, 7),
        scratch=(
            pltpu.VMEM(leaf_rhs.shape, BF16),
            pltpu.VMEM(leaf_update.shape, BF16),
            pltpu.VMEM(leaf_inv.shape, BF16),
            pltpu.SemaphoreType.DMA((3,)),
        ),
    )(me, leaf_cols, own_rows, arrived, value, leaf_rhs, leaf_update, leaf_inv)
    return (sep_out, leaf_out)


def solution(mesh):
    finer = Mesh(mesh.devices.reshape(mesh.shape["grp"], 4, 4, 2), ALL)
    split = P(ALL, None)
    in_specs = (split, split, split, P("grp", None), split, split, split, split, P(ALL), split)
    return jax.shard_map(
        on_device, mesh=finer, in_specs=in_specs, out_specs=(split, split), check_vma=False
    )
```

```python
import functools

import jax
import jax.numpy as jnp
from jax import lax
from jax.experimental import pallas as pl
from jax.experimental.pallas import tpu as pltpu
from jax.sharding import Mesh
from jax.sharding import PartitionSpec as P

ALL = ("grp", "x_1", "x_0", "y_1", "y_0", "core")
XY = ("y_0", "x_0", "y_1", "x_1")
SLOTS, LIST = 64, 8
BASE = 64
CORE = "core"
BF16, F32, I32 = jnp.bfloat16, jnp.float32, jnp.int32
MIB = 1 << 20


def to_all(blocks, axes):
    return lax.all_to_all(blocks, axes, 0, 0, tiled=True)


def swapped(value):
    return lax.ppermute(value, CORE, [(0, 1), (1, 0)])


def dot(a, b, dims=((1,), (0,))):
    return lax.dot_general(a, b, (dims, ((), ())), preferred_element_type=F32)


def column(row):
    size = 128
    eye = lax.broadcasted_iota(I32, (size, size), 0) == lax.broadcasted_iota(I32, (size, size), 1)
    parts = [
        jnp.sum(jnp.where(eye, row[:, i : i + size], F32(0.0)), axis=1, keepdims=True)
        for i in range(0, row.shape[1], size)
    ]
    return jnp.concatenate(parts, axis=0)


def chosen(places, lines):
    if places.shape[0] == 1:
        places = column(places.astype(F32)).astype(I32)
    at = lax.broadcasted_iota(I32, (places.shape[0], lines), 1)
    return jnp.where(at == places, F32(1.0), F32(0.0)).astype(BF16)


def kernel_call(body, outs, flops, n_bytes, in_smem=(), limit=16, in_hbm=(), out_hbm=(), scratch=()):
    def call(*args):
        specs = [
            pl.BlockSpec(
                memory_space=pltpu.SMEM if i in in_smem else pltpu.HBM if i in in_hbm else pltpu.VMEM
            )
            for i in range(len(args))
        ]
        return pl.pallas_call(
            body,
            out_shape=outs,
            in_specs=specs,
            out_specs=jax.tree.unflatten(
                jax.tree.structure(outs),
                [
                    pl.BlockSpec(
                        memory_space=pltpu.SMEM
                        if out.ndim == 1
                        else pltpu.HBM
                        if i in out_hbm
                        else pltpu.VMEM
                    )
                    for i, out in enumerate(jax.tree.leaves(outs))
                ],
            ),
            scratch_shapes=scratch,
            cost_estimate=pl.CostEstimate(
                flops=flops, bytes_accessed=n_bytes, transcendentals=0
            ),
            compiler_params=pltpu.CompilerParams(vmem_limit_bytes=int(limit * MIB)),
        )(*args)

    return call


def log2(size):
    assert size & (size - 1) == 0
    return size.bit_length() - 1


def spot(chip):
    bits = [(chip >> i) & 1 for i in range(4)]
    return (bits[0] << 3) + (bits[2] << 2) + (bits[1] << 1) + bits[3]


def root_owner(rows, own, cores, devices, groups):
    device = (rows >> log2(own)) & (devices - 1)
    group = rows >> log2(own * devices)
    line = ((device & (cores - 1)) << log2(groups)) + group
    return spot(device >> log2(cores)), (line << log2(own)) + (rows & (own - 1))


def ancestor_owner(sizes, sep, held, rows):
    chip, line = root_owner(rows - sep, *sizes)
    here = rows < sep
    return jnp.where(here, spot(rows >> log2(held)), chip), jnp.where(here, rows & (held - 1), held + line)


def before(size):
    lines = lax.broadcasted_iota(I32, (size, size), 0)
    return one(lines < lax.broadcasted_iota(I32, (size, size), 1))


def one(mask):
    return jnp.where(mask, F32(1.0), F32(0.0)).astype(BF16)


def encoded(rows):
    digits = [rows >> log2(BASE), rows & (BASE - 1)]
    size = 128
    lines = [d[:, i : i + size] for d in digits for i in range(0, rows.shape[1], size)]
    return jnp.concatenate(lines, axis=0).astype(F32).astype(BF16)


def decoded(lines):
    value = lines.astype(F32)
    half = value.shape[0] // 2
    value = value[:half] * F32(BASE) + value[half:]
    return jnp.concatenate([value[i : i + 1] for i in range(half)], axis=1).astype(I32)


def side(first, value):
    half = value.shape[1] // 2
    return jnp.where(first, value[:, :half], value[:, half:])


def of_core(first, value):
    half = value.shape[0] // 2
    return jnp.where(first, value[:half], value[half:])


def joined(first, mine, theirs):
    return jnp.concatenate(
        [jnp.where(first, mine, theirs), jnp.where(first, theirs, mine)], axis=1
    )


def fan_body(root, out):
    half = root.shape[1] // 2
    low, high = root[:, :half], root[:, half:]
    groups = out.shape[0] // 2
    for i in range(groups):
        out[i] = low
        out[groups + i] = high


def pack_body(core, rhs, update, leaf_rows, out):
    rows, half = rhs.shape[0], rhs.shape[1] // 2
    out[:rows, :half] = side(core[0] != 0, rhs[...])
    out[:rows, half:] = update[...]
    listed = leaf_rows[...]
    digits = jnp.concatenate([listed >> log2(BASE), listed & (BASE - 1)], axis=1)
    spare = out.shape[0] - rows
    digits = jnp.broadcast_to(digits.astype(F32), (spare, digits.shape[1]))
    out[rows:, : digits.shape[1]] = digits.astype(BF16)
    out[rows:, digits.shape[1] :] = jnp.zeros((spare, out.shape[1] - digits.shape[1]), BF16)


def plan_body(
    sizes, me, rows, rhs, update, leaf_rows, arrived, rhs_out, spread_out, select_out, list_out, fits_out
):
    own, half = rhs.shape[0], rhs.shape[1] // 2
    core, chip = me[0], me[1]
    rhs_out[...] = jnp.concatenate([side(core == 0, rhs[...]), arrived[:own, :half]], axis=0)
    both = jnp.concatenate([update[...], arrived[:own, half:]], axis=0)

    chips = spread_out.shape[1] // SLOTS
    wanted = rows[...]
    size = wanted.shape[1]
    owner, line = root_owner(wanted, *sizes)
    owned = lax.broadcasted_iota(I32, (chips, size), 0) == owner
    rank = jnp.where(owned, dot(one(owned), before(size)), F32(0.0))
    rank = jnp.sum(rank, axis=0, keepdims=True).astype(I32)
    most = jnp.max(rank.astype(F32))
    fits = (most < F32(SLOTS)).astype(I32)
    fits_out[0] = fits
    place = jnp.where(fits == 1, owner * SLOTS + rank, lax.broadcasted_iota(I32, (1, size), 1))
    spread_out[...] = dot(both, chosen(place, spread_out.shape[1])).astype(BF16)

    mine = jnp.where(owner == chip, rank, -1)
    slot = one(lax.broadcasted_iota(I32, (SLOTS, size), 0) == mine)
    lines = select_out.shape[1]
    source = one(lax.broadcasted_iota(I32, (lines, size), 0) == line)
    select_out[...] = dot(slot, source, ((1,), (1,))).astype(BF16)

    n_leaf = leaf_rows.shape[1]
    digits = arrived[own:, : 2 * n_leaf].astype(F32)[:1]
    other = (digits[:, :n_leaf] * F32(BASE) + digits[:, n_leaf:]).astype(I32)
    list_out[...] = encoded(jnp.concatenate([leaf_rows[...], other], axis=1))


def select_body(select, lines, listed, out):
    rows = dot(select[...], lines[...]).astype(BF16)
    listed = listed[...]
    for i in range(out.shape[0]):
        out[i, :SLOTS] = rows
        out[i, SLOTS:] = listed


def all_lines_body(lines, listed, out):
    held = lines.shape[0]
    for i in range(out.shape[0]):
        out[i, :held] = lines[...]
        out[i, held:] = listed[...]


def all_rows_body(sizes, rows, arrived, out):
    chips, held, wide = arrived.shape
    held = held - LIST
    owner, line = root_owner(rows[...], *sizes)
    table = arrived[:, :held].reshape(chips * held, wide)
    picked = dot(chosen(owner * held + line, chips * held), table).astype(BF16)
    full = picked.shape[0] // SLOTS
    out[:full, :SLOTS] = picked.reshape(full, SLOTS, wide)
    if chips > full:
        out[full:, :SLOTS] = jnp.zeros((chips - full, SLOTS, wide), BF16)
    out[:, SLOTS:] = arrived[:, held:]


def terms_body(
    rhs, spread, arrived, own_inverse_at, other_inverse_at, out, own_inverse, other_inverse, block, sems
):
    copies = (
        pltpu.make_async_copy(own_inverse_at, own_inverse, sems.at[0]),
        pltpu.make_async_copy(other_inverse_at, other_inverse, sems.at[1]),
    )
    for copy in copies:
        copy.start()
    chips, _, width = out.shape
    wide = rhs.shape[1]
    table = arrived[:, :SLOTS].reshape(chips * SLOTS, wide)
    residual = rhs[...].astype(F32) - dot(spread[...], table)
    residual = residual.astype(BF16).astype(F32).T.astype(BF16)
    for copy in copies:
        copy.wait()
    sent = []
    for chip in range(chips):
        i = spot(chip)
        at = slice(chip * width, (chip + 1) * width)
        both = jnp.concatenate([own_inverse[:, at], other_inverse[:, at]], axis=0)
        block[i] = dot(residual, both).astype(BF16)
        sent.append(pltpu.make_async_copy(block.at[i], out.at[i], sems.at[2 + i]))
        sent[-1].start()
    for copy in sent:
        copy.wait()


def leaf_plan_body(sizes, sep, held, me, arrived, select_out, place_out, fits_out, mine_at, line_at):
    chips = arrived.shape[0]
    chip = me[1]
    rows = jnp.concatenate([decoded(arrived[i, SLOTS:]) for i in range(chips)], axis=0)
    size = rows.shape[1]
    owner, line = ancestor_owner(sizes, sep, held, rows)
    counts = before(size)
    owned = jnp.concatenate([owner == i for i in range(chips)], axis=0)
    rank = jnp.where(owned, dot(one(owned), counts), F32(0.0))
    fits = (jnp.max(rank) < F32(SLOTS)).astype(I32)
    fits_out[0] = fits

    listed = lax.broadcasted_iota(I32, (chips, 1), 0) == chip
    own_rank = jnp.zeros((1, size), F32)
    for i in range(chips):
        part = rank[i * chips : (i + 1) * chips]
        own_rank = own_rank + jnp.sum(jnp.where(listed, part, F32(0.0)), axis=0, keepdims=True)
    own_owner = jnp.sum(jnp.where(listed, owner.astype(F32), F32(0.0)), axis=0, keepdims=True)
    place = own_owner * F32(SLOTS) + own_rank
    place = jnp.where(fits == 1, place, lax.broadcasted_iota(I32, (1, size), 1).astype(F32))
    place_out[...] = column(place).astype(I32)

    mine = owner == chip
    mine_at[...] = jnp.where(mine, dot(one(mine), counts), F32(-1.0)).astype(I32)
    line_at[...] = line

    def step(i, _):
        slot = one(lax.broadcasted_iota(I32, (SLOTS, size), 0) == mine_at[pl.ds(i, 1), :])
        lines = select_out.shape[2]
        source = one(lax.broadcasted_iota(I32, (lines, size), 0) == line_at[pl.ds(i, 1), :])
        select_out[i] = dot(slot, source, ((1,), (1,))).astype(BF16)
        return 0

    lax.fori_loop(0, chips, step, 0)


def sum_body(terms, select, lines, out, blocks):
    total = terms[0].astype(F32)
    for i in range(1, terms.shape[0]):
        total = total + terms[i].astype(F32)
    value = total.T.astype(BF16)
    out[...] = value
    table = jnp.concatenate([value, lines[...]], axis=0)
    chips, slots, size = select.shape
    rows = dot(select[...].reshape(chips * slots, size), table).astype(BF16)
    blocks[...] = rows.reshape(blocks.shape)


def all_ancestors_body(sizes, sep, held, listed, arrived, out):
    chips, lines, wide = arrived.shape
    owner, line = ancestor_owner(sizes, sep, held, decoded(listed[...]))
    place = owner * lines + line
    total = jnp.zeros((place.shape[1], wide), F32)
    for i in range(chips):
        total = total + dot(chosen(place - i * lines, lines), arrived[i])
    full = total.shape[0] // SLOTS
    out[:full] = total.astype(BF16).reshape(full, SLOTS, wide)
    if chips > full:
        out[full:] = jnp.zeros((chips - full, SLOTS, wide), BF16)


def ancestors_body(me, place, arrived, value, own, sent):
    chips, slots, wide = arrived.shape
    table = arrived[...].reshape(chips * slots, wide)
    rows = dot(chosen(place[...], chips * slots), table).astype(BF16)
    half = rows.shape[0] // 2
    own[...] = rows[:half]
    sent[:half] = rows[half:]
    sent[half:] = of_core(me[0] != 0, value[...])


def leaf_body(me, cols, own, arrived, value, rhs, update, inverse, out, sep_out, block, sems):
    first, half = me[0] == 0, own.shape[0]
    rows = joined(first, own[...], arrived[:half])
    live = lax.broadcasted_iota(I32, out.shape, 0) < cols[0]
    residual = rhs[...].astype(F32) - dot(update[...], rows)
    residual = jnp.where(live, residual, F32(0.0)).astype(BF16)
    size = out.shape[0] // sems.shape[0]
    sent = []
    for i in range(sems.shape[0]):
        at = pl.ds(i * size, size)
        solved = dot(inverse[at, :], residual)
        live = lax.broadcasted_iota(I32, solved.shape, 0) < cols[0] - i * size
        block[at, :] = jnp.where(live, solved, F32(0.0)).astype(BF16)
        sent.append(pltpu.make_async_copy(block.at[at], out.at[at], sems.at[i]))
        sent[-1].start()
    sep_out[...] = joined(first, of_core(first, value[...]), arrived[half:])
    for copy in sent:
        copy.wait()


def on_device(
    root_solution,
    sep_rhs,
    sep_update,
    sep_rows,
    sep_inv_cols,
    leaf_rhs,
    leaf_update,
    leaf_rows,
    leaf_cols,
    leaf_inv,
):
    groups = lax.axis_size("grp")
    chips = lax.axis_size(XY)
    cores = lax.axis_size(CORE)
    devices = chips * cores
    me = jnp.stack([lax.axis_index(CORE), lax.axis_index(XY)]).astype(I32)
    own_root, nrhs = root_solution.shape
    own_sep, sep = sep_inv_cols.shape
    wide = nrhs // cores
    n_sep, n_leaf = sep_rows.shape[1], leaf_rows.shape[1]
    held = cores * own_sep
    lines_here = groups * cores * own_root
    sizes = (own_root, cores, devices, groups)

    def array(*shape, dtype=BF16):
        return jax.ShapeDtypeStruct(shape, dtype)

    flag = array(1, dtype=I32)

    blocks = kernel_call(fan_body, array(groups * cores, own_root, wide), 1024, MIB, limit=4)(
        root_solution
    )
    lines = to_all(blocks, (CORE, "grp")).reshape(lines_here, wide)

    other_inverse = swapped(sep_inv_cols)
    sent = kernel_call(
        pack_body, array(own_sep + 8, wide + n_sep), own_sep, MIB, (0,), 4
    )(me, sep_rhs, sep_update, leaf_rows)
    arrived = swapped(sent)

    rhs, spread, select, listed, fits = kernel_call(
        functools.partial(plan_body, sizes),
        (
            array(held, wide),
            array(held, chips * SLOTS),
            array(SLOTS, lines_here),
            array(LIST, 128),
            flag,
        ),
        2 * held * n_sep * chips * SLOTS,
        MIB,
        (0,),
    )(me, sep_rows, sep_rhs, sep_update, leaf_rows, arrived)

    mail = array(chips, SLOTS + LIST, wide)
    blocks = kernel_call(select_body, mail, SLOTS * lines_here * wide, MIB, limit=4)(
        select, lines, listed
    )

    def few_rows(blocks, lines, listed, sep_rows):
        return to_all(blocks, XY)

    def all_rows(blocks, lines, listed, sep_rows):
        full = array(chips, lines_here + LIST, wide)
        full = kernel_call(all_lines_body, full, 1024, 2 * MIB)(lines, listed)
        return kernel_call(functools.partial(all_rows_body, sizes), mail, 1024, 2 * MIB)(sep_rows, to_all(full, XY))

    root_rows = lax.cond(fits[0] == 1, few_rows, all_rows, blocks, lines, listed, sep_rows)

    terms = kernel_call(
        terms_body,
        array(chips, wide, sep // chips),
        2 * held * wide * (chips * SLOTS + sep),
        6 * MIB,
        in_hbm=(3, 4),
        out_hbm=(0,),
        scratch=(
            pltpu.VMEM(sep_inv_cols.shape, BF16),
            pltpu.VMEM(sep_inv_cols.shape, BF16),
            pltpu.VMEM((chips, wide, sep // chips), BF16),
            pltpu.SemaphoreType.DMA((2 + chips,)),
        ),
    )(rhs, spread, root_rows, sep_inv_cols, other_inverse)
    terms = to_all(terms, XY)

    select, place, fits = kernel_call(
        functools.partial(leaf_plan_body, sizes, sep, held),
        (
            array(chips, SLOTS, held + lines_here),
            array(cores * n_leaf, 1, dtype=I32),
            flag,
        ),
        chips * 2**26,
        2 * MIB,
        (0,),
        scratch=(
            pltpu.VMEM((chips, cores * n_leaf), I32),
            pltpu.VMEM((chips, cores * n_leaf), I32),
        ),
    )(me, root_rows)
    mail = array(chips, SLOTS, wide)
    value, blocks = kernel_call(
        sum_body, (array(held, wide), mail), 2 * chips * SLOTS * wide * (held + lines_here), 2 * MIB
    )(terms, select, lines)

    def few_ancestors(blocks, value, lines, listed):
        return to_all(blocks, XY)

    def all_ancestors(blocks, value, lines, listed):
        table = jnp.concatenate([value, lines], axis=0)
        table = to_all(jnp.broadcast_to(table, (chips, *table.shape)), XY)
        return kernel_call(functools.partial(all_ancestors_body, sizes, sep, held), mail, 1024, 2 * MIB)(listed, table)

    ancestors = lax.cond(fits[0] == 1, few_ancestors, all_ancestors, blocks, value, lines, listed)

    own_rows, sent = kernel_call(
        ancestors_body,
        (array(n_leaf, wide), array(n_leaf + own_sep, wide)),
        2 * cores * n_leaf * wide * chips * SLOTS,
        MIB,
        (0,),
    )(me, place, ancestors, value)
    arrived = swapped(sent)
    leaf_out, sep_out = kernel_call(
        leaf_body,
        (array(*leaf_rhs.shape), array(own_sep, nrhs)),
        2 * nrhs * (leaf_inv.size + leaf_update.size),
        4 * MIB,
        (0, 1),
        out_hbm=(0,),
        scratch=(pltpu.VMEM(leaf_rhs.shape, BF16), pltpu.SemaphoreType.DMA((4,))),
    )(me, leaf_cols, own_rows, arrived, value, leaf_rhs, leaf_update, leaf_inv)
    return (sep_out, leaf_out)


def solution(mesh):
    finer = Mesh(mesh.devices.reshape(mesh.shape["grp"], 2, 2, 2, 2, 2), ALL)
    split = P(ALL, None)
    in_specs = (split, split, split, P("grp", None), split, split, split, split, P(ALL), split)
    return jax.shard_map(
        on_device, mesh=finer, in_specs=in_specs, out_specs=(split, split), check_vma=False
    )
```

```python
import functools

import jax
import jax.numpy as jnp
from jax import lax
from jax.experimental import pallas as pl
from jax.experimental.pallas import tpu as pltpu
from jax.sharding import Mesh
from jax.sharding import PartitionSpec as P

ALL = ("grp", "x_1", "x_0", "y_1", "y_0", "core")
XY = ("y_0", "x_0", "y_1", "x_1")
SLOTS, LIST = 64, 8
BASE = 64
CORE = "core"
BF16, F32, I32 = jnp.bfloat16, jnp.float32, jnp.int32
MIB = 1 << 20


def to_all(blocks, axes):
    return lax.all_to_all(blocks, axes, 0, 0, tiled=True)


def swapped(value):
    return lax.ppermute(value, CORE, [(0, 1), (1, 0)])


def dot(a, b, dims=((1,), (0,))):
    return lax.dot_general(a, b, (dims, ((), ())), preferred_element_type=F32)


def column(row):
    size = 128
    eye = lax.broadcasted_iota(I32, (size, size), 0) == lax.broadcasted_iota(I32, (size, size), 1)
    parts = [
        jnp.sum(jnp.where(eye, row[:, i : i + size], F32(0.0)), axis=1, keepdims=True)
        for i in range(0, row.shape[1], size)
    ]
    return jnp.concatenate(parts, axis=0)


def chosen(places, lines):
    if places.shape[0] == 1:
        places = column(places.astype(F32)).astype(I32)
    at = lax.broadcasted_iota(I32, (places.shape[0], lines), 1)
    return jnp.where(at == places, F32(1.0), F32(0.0)).astype(BF16)


def kernel_call(body, outs, flops, n_bytes, in_smem=(), limit=16, in_hbm=(), out_hbm=(), scratch=()):
    def call(*args):
        specs = [
            pl.BlockSpec(
                memory_space=pltpu.SMEM if i in in_smem else pltpu.HBM if i in in_hbm else pltpu.VMEM
            )
            for i in range(len(args))
        ]
        return pl.pallas_call(
            body,
            out_shape=outs,
            in_specs=specs,
            out_specs=jax.tree.unflatten(
                jax.tree.structure(outs),
                [
                    pl.BlockSpec(
                        memory_space=pltpu.SMEM
                        if out.ndim == 1
                        else pltpu.HBM
                        if i in out_hbm
                        else pltpu.VMEM
                    )
                    for i, out in enumerate(jax.tree.leaves(outs))
                ],
            ),
            scratch_shapes=scratch,
            cost_estimate=pl.CostEstimate(flops=flops, bytes_accessed=n_bytes, transcendentals=0),
            compiler_params=pltpu.CompilerParams(vmem_limit_bytes=int(limit * MIB)),
        )(*args)

    return call


def log2(size):
    assert size & (size - 1) == 0
    return size.bit_length() - 1


def spot(chip):
    bits = [(chip >> i) & 1 for i in range(4)]
    return (bits[0] << 3) + (bits[2] << 2) + (bits[1] << 1) + bits[3]


def root_owner(rows, own, cores, devices, groups):
    device = (rows >> log2(own)) & (devices - 1)
    group = rows >> log2(own * devices)
    line = ((device & (cores - 1)) << log2(groups)) + group
    return spot(device >> log2(cores)), (line << log2(own)) + (rows & (own - 1))


def ancestor_owner(sizes, sep, held, rows):
    chip, line = root_owner(rows - sep, *sizes)
    here = rows < sep
    return jnp.where(here, spot(rows >> log2(held)), chip), jnp.where(here, rows & (held - 1), held + line)


def before(size):
    lines = lax.broadcasted_iota(I32, (size, size), 0)
    return one(lines < lax.broadcasted_iota(I32, (size, size), 1))


def one(mask):
    return jnp.where(mask, F32(1.0), F32(0.0)).astype(BF16)


def encoded(rows):
    digits = [rows >> log2(BASE), rows & (BASE - 1)]
    size = 128
    lines = [d[:, i : i + size] for d in digits for i in range(0, rows.shape[1], size)]
    return jnp.concatenate(lines, axis=0).astype(F32).astype(BF16)


def decoded(lines):
    value = lines.astype(F32)
    half = value.shape[0] // 2
    value = value[:half] * F32(BASE) + value[half:]
    return jnp.concatenate([value[i : i + 1] for i in range(half)], axis=1).astype(I32)


def side(first, value):
    half = value.shape[1] // 2
    return jnp.where(first, value[:, :half], value[:, half:])


def of_core(first, value):
    half = value.shape[0] // 2
    return jnp.where(first, value[:half], value[half:])


def joined(first, mine, theirs):
    return jnp.concatenate(
        [jnp.where(first, mine, theirs), jnp.where(first, theirs, mine)], axis=1
    )


def fan_body(root, out):
    half = root.shape[1] // 2
    low, high = root[:, :half], root[:, half:]
    groups = out.shape[0] // 2
    for i in range(groups):
        out[i] = low
        out[groups + i] = high


def pack_body(
    core, rhs_at, update_at, rows_at, leaf_rows_at, out, kept, rhs, update, wanted, listed, sems
):
    pairs = ((rhs_at, rhs), (update_at, update), (rows_at, wanted), (leaf_rows_at, listed))
    fetches = [pltpu.make_async_copy(*pair, sems.at[i]) for i, pair in enumerate(pairs)]
    for fetch in fetches:
        fetch.start()
    for fetch in fetches:
        fetch.wait()
    rows, half = rhs.shape[0], rhs.shape[1] // 2
    first = core[0] == 0
    width = update.shape[1]
    leaf, sep = listed[...], wanted[...]
    digits = [
        jnp.concatenate([leaf >> log2(BASE), leaf & (BASE - 1)], axis=1),
        sep >> log2(BASE),
        sep & (BASE - 1),
    ]
    digits = jnp.concatenate(digits + [jnp.zeros((LIST - 3, width), I32)], axis=0)
    digits = digits.astype(F32).astype(BF16)
    for target, take in ((out, jnp.logical_not(first)), (kept, first)):
        target[:rows, :half] = side(take, rhs[...])
        target[:rows, half:] = update[...]
        target[rows:, :half] = jnp.zeros((LIST, half), BF16)
        target[rows:, half:] = digits


def plan_body(
    sizes, chip_at, kept, arrived, rhs_out, spread_out, select_out, list_out, fits_out
):
    own, half = kept.shape[0] - LIST, rhs_out.shape[1]
    chip = chip_at[0]
    rhs_out[...] = jnp.concatenate([kept[:own, :half], arrived[:own, :half]], axis=0)
    both = jnp.concatenate([kept[:own, half:], arrived[:own, half:]], axis=0)
    digits, other_digits = kept[own:, half:].astype(F32), arrived[own:, half:].astype(F32)

    chips = spread_out.shape[1] // SLOTS
    wanted = (digits[1:2] * F32(BASE) + digits[2:3]).astype(I32)
    size = wanted.shape[1]
    owner, line = root_owner(wanted, *sizes)
    owned = lax.broadcasted_iota(I32, (chips, size), 0) == owner
    rank = jnp.where(owned, dot(one(owned), before(size)), F32(0.0))
    rank = jnp.sum(rank, axis=0, keepdims=True).astype(I32)
    most = jnp.max(rank.astype(F32))
    fits = (most < F32(SLOTS)).astype(I32)
    fits_out[0] = fits
    place = jnp.where(fits == 1, owner * SLOTS + rank, lax.broadcasted_iota(I32, (1, size), 1))
    spread_out[...] = dot(both, chosen(place, spread_out.shape[1])).astype(BF16)

    mine = jnp.where(owner == chip, rank, -1)
    slot = one(lax.broadcasted_iota(I32, (SLOTS, size), 0) == mine)
    lines = select_out.shape[1]
    source = one(lax.broadcasted_iota(I32, (lines, size), 0) == line)
    select_out[...] = dot(slot, source, ((1,), (1,))).astype(BF16)

    listed = []
    for line in (digits[:1], other_digits[:1]):
        n_leaf = line.shape[1] // 2
        listed.append((line[:, :n_leaf] * F32(BASE) + line[:, n_leaf:]).astype(I32))
    list_out[...] = encoded(jnp.concatenate(listed, axis=1))


def select_body(select, lines, listed, out):
    rows = dot(select[...], lines[...]).astype(BF16)
    listed = listed[...]
    for i in range(out.shape[0]):
        out[i, :SLOTS] = rows
        out[i, SLOTS:] = listed


def all_lines_body(lines, listed, out):
    held = lines.shape[0]
    for i in range(out.shape[0]):
        out[i, :held] = lines[...]
        out[i, held:] = listed[...]


def all_rows_body(sizes, rows, arrived, out):
    chips, held, wide = arrived.shape
    held = held - LIST
    owner, line = root_owner(rows[...], *sizes)
    table = arrived[:, :held].reshape(chips * held, wide)
    picked = dot(chosen(owner * held + line, chips * held), table).astype(BF16)
    full = picked.shape[0] // SLOTS
    out[:full, :SLOTS] = picked.reshape(full, SLOTS, wide)
    if chips > full:
        out[full:, :SLOTS] = jnp.zeros((chips - full, SLOTS, wide), BF16)
    out[:, SLOTS:] = arrived[:, held:]


def terms_body(rhs, spread, arrived, own_inverse_at, other_inverse_at, out, own_inverse, other_inverse, sems):
    copies = (
        pltpu.make_async_copy(own_inverse_at, own_inverse, sems.at[0]),
        pltpu.make_async_copy(other_inverse_at, other_inverse, sems.at[1]),
    )
    for copy in copies:
        copy.start()
    chips, _, width = out.shape
    wide = rhs.shape[1]
    table = arrived[:, :SLOTS].reshape(chips * SLOTS, wide)
    residual = rhs[...].astype(F32) - dot(spread[...], table)
    residual = residual.astype(BF16).astype(F32).T.astype(BF16)
    for copy in copies:
        copy.wait()
    for i in range(chips):
        at = slice(i * width, (i + 1) * width)
        both = jnp.concatenate([own_inverse[:, at], other_inverse[:, at]], axis=0)
        out[spot(i)] = dot(residual, both).astype(BF16)


def leaf_plan_body(sizes, sep, held, chip_at, arrived, select_out, place_out, fits_out, mine_at, line_at):
    chips = arrived.shape[0]
    chip = chip_at[0]
    rows = jnp.concatenate([decoded(arrived[i, SLOTS:]) for i in range(chips)], axis=0)
    size = rows.shape[1]
    owner, line = ancestor_owner(sizes, sep, held, rows)
    counts = before(size)
    owned = jnp.concatenate([owner == i for i in range(chips)], axis=0)
    rank = jnp.where(owned, dot(one(owned), counts), F32(0.0))
    fits = (jnp.max(rank) < F32(SLOTS)).astype(I32)
    fits_out[0] = fits

    listed = lax.broadcasted_iota(I32, (chips, 1), 0) == chip
    own_rank = jnp.zeros((1, size), F32)
    for i in range(chips):
        part = rank[i * chips : (i + 1) * chips]
        own_rank = own_rank + jnp.sum(jnp.where(listed, part, F32(0.0)), axis=0, keepdims=True)
    own_owner = jnp.sum(jnp.where(listed, owner.astype(F32), F32(0.0)), axis=0, keepdims=True)
    place = own_owner * F32(SLOTS) + own_rank
    place = jnp.where(fits == 1, place, lax.broadcasted_iota(I32, (1, size), 1).astype(F32))
    place_out[...] = place.astype(I32)

    mine = owner == chip
    mine_at[...] = jnp.where(mine, dot(one(mine), counts), F32(-1.0)).astype(I32)
    line_at[...] = line

    def step(i, _):
        slot = one(lax.broadcasted_iota(I32, (SLOTS, size), 0) == mine_at[pl.ds(i, 1), :])
        lines = select_out.shape[2]
        source = one(lax.broadcasted_iota(I32, (lines, size), 0) == line_at[pl.ds(i, 1), :])
        select_out[i] = dot(slot, source, ((1,), (1,))).astype(BF16)
        return 0

    lax.fori_loop(0, chips, step, 0)


def sum_body(terms, select, lines, out, blocks):
    total = terms[0].astype(F32)
    for i in range(1, terms.shape[0]):
        total = total + terms[i].astype(F32)
    value = total.T.astype(BF16)
    out[...] = value
    table = jnp.concatenate([value, lines[...]], axis=0)
    chips, slots, size = select.shape
    rows = dot(select[...].reshape(chips * slots, size), table).astype(BF16)
    blocks[...] = rows.reshape(blocks.shape)


def all_ancestors_body(sizes, sep, held, listed, arrived, out):
    chips, lines, wide = arrived.shape
    owner, line = ancestor_owner(sizes, sep, held, decoded(listed[...]))
    place = owner * lines + line
    total = jnp.zeros((place.shape[1], wide), F32)
    for i in range(chips):
        total = total + dot(chosen(place - i * lines, lines), arrived[i])
    full = total.shape[0] // SLOTS
    out[:full] = total.astype(BF16).reshape(full, SLOTS, wide)
    if chips > full:
        out[full:] = jnp.zeros((chips - full, SLOTS, wide), BF16)


def ancestors_body(core, place, arrived, value, rhs_at, update_at, own, sent, rhs, update, sems):
    fetches = [
        pltpu.make_async_copy(update_at, update, sems.at[0]),
        pltpu.make_async_copy(rhs_at, rhs, sems.at[1]),
    ]
    for fetch in fetches:
        fetch.start()
    chips, slots, wide = arrived.shape
    table = arrived[...].reshape(chips * slots, wide)
    rows = dot(chosen(place[...], chips * slots), table).astype(BF16)
    half = rows.shape[0] // 2
    own[...] = rows[:half]
    sent[:half] = rows[half:]
    sent[half:] = of_core(core[0] != 0, value[...])
    for fetch in fetches:
        fetch.wait()


def leaf_body(core, cols, own, arrived, value, rhs, update, inverse, out, sep_out, block, sems):
    first, half = core[0] == 0, own.shape[0]
    rows = joined(first, own[...], arrived[:half])
    live = lax.broadcasted_iota(I32, out.shape, 0) < cols[0]
    residual = rhs[...].astype(F32) - dot(update[...], rows)
    residual = jnp.where(live, residual, F32(0.0)).astype(BF16)
    size = out.shape[0] // sems.shape[0]
    sent = []
    for i in range(sems.shape[0]):
        at = pl.ds(i * size, size)
        solved = dot(inverse[at, :], residual)
        live = lax.broadcasted_iota(I32, solved.shape, 0) < cols[0] - i * size
        block[at, :] = jnp.where(live, solved, F32(0.0)).astype(BF16)
        sent.append(pltpu.make_async_copy(block.at[at], out.at[at], sems.at[i]))
        sent[-1].start()
    sep_out[...] = joined(first, of_core(first, value[...]), arrived[half:])
    for copy in sent:
        copy.wait()


def on_device(
    root_solution,
    sep_rhs,
    sep_update,
    sep_rows,
    sep_inv_cols,
    leaf_rhs,
    leaf_update,
    leaf_rows,
    leaf_cols,
    leaf_inv,
):
    groups = lax.axis_size("grp")
    chips = lax.axis_size(XY)
    cores = lax.axis_size(CORE)
    devices = chips * cores
    core, chip = lax.axis_index(CORE).astype(I32)[None], lax.axis_index(XY).astype(I32)[None]
    own_root, nrhs = root_solution.shape
    own_sep, sep = sep_inv_cols.shape
    wide = nrhs // cores
    n_sep, n_leaf = sep_rows.shape[1], leaf_rows.shape[1]
    held = cores * own_sep
    lines_here = groups * cores * own_root
    sizes = (own_root, cores, devices, groups)

    def array(*shape, dtype=BF16):
        return jax.ShapeDtypeStruct(shape, dtype)

    flag = array(1, dtype=I32)

    blocks = kernel_call(fan_body, array(groups * cores, own_root, wide), 1024, MIB, limit=4)(
        root_solution
    )
    lines = to_all(blocks, (CORE, "grp")).reshape(lines_here, wide)

    other_inverse = swapped(sep_inv_cols)
    assert n_sep == 2 * n_leaf
    sent, kept = kernel_call(
        pack_body,
        (array(own_sep + LIST, wide + n_sep), array(own_sep + LIST, wide + n_sep)),
        own_sep,
        MIB,
        (0,),
        63.25,
        in_hbm=(1, 2, 3, 4),
        scratch=(
            pltpu.VMEM(sep_rhs.shape, BF16),
            pltpu.VMEM(sep_update.shape, BF16),
            pltpu.VMEM(sep_rows.shape, I32),
            pltpu.VMEM(leaf_rows.shape, I32),
            pltpu.SemaphoreType.DMA((4,)),
        ),
    )(core, sep_rhs, sep_update, sep_rows, leaf_rows)
    arrived = swapped(sent)

    rhs, spread, select, listed, fits = kernel_call(
        functools.partial(plan_body, sizes),
        (
            array(held, wide),
            array(held, chips * SLOTS),
            array(SLOTS, lines_here),
            array(LIST, 128),
            flag,
        ),
        2 * held * n_sep * chips * SLOTS,
        MIB,
        (0,),
    )(chip, kept, arrived)

    mail = array(chips, SLOTS + LIST, wide)
    blocks = kernel_call(select_body, mail, SLOTS * lines_here * wide, MIB, limit=4)(
        select, lines, listed
    )

    def few_rows(blocks, lines, listed, sep_rows):
        return to_all(blocks, XY)

    def all_rows(blocks, lines, listed, sep_rows):
        full = array(chips, lines_here + LIST, wide)
        full = kernel_call(all_lines_body, full, 1024, 2 * MIB)(lines, listed)
        return kernel_call(
            functools.partial(all_rows_body, sizes), mail, 1024, 2 * MIB
        )(sep_rows, to_all(full, XY))

    root_rows = lax.cond(fits[0] == 1, few_rows, all_rows, blocks, lines, listed, sep_rows)

    terms = kernel_call(
        terms_body,
        array(chips, wide, sep // chips),
        2 * held * wide * (chips * SLOTS + sep),
        6 * MIB,
        in_hbm=(3, 4),
        scratch=(
            pltpu.VMEM(sep_inv_cols.shape, BF16),
            pltpu.VMEM(sep_inv_cols.shape, BF16),
            pltpu.SemaphoreType.DMA((2,)),
        ),
    )(rhs, spread, root_rows, sep_inv_cols, other_inverse)
    terms = to_all(terms, XY)

    select, place, fits = kernel_call(
        functools.partial(leaf_plan_body, sizes, sep, held),
        (
            array(chips, SLOTS, held + lines_here),
            array(1, cores * n_leaf, dtype=I32),
            flag,
        ),
        chips * 2**26,
        2 * MIB,
        (0,),
        scratch=(
            pltpu.VMEM((chips, cores * n_leaf), I32),
            pltpu.VMEM((chips, cores * n_leaf), I32),
        ),
    )(chip, root_rows)
    mail = array(chips, SLOTS, wide)
    value, blocks = kernel_call(
        sum_body, (array(held, wide), mail), 2 * chips * SLOTS * wide * (held + lines_here), 2 * MIB
    )(terms, select, lines)

    def few_ancestors(blocks, value, lines, listed):
        return to_all(blocks, XY)

    def all_ancestors(blocks, value, lines, listed):
        table = jnp.concatenate([value, lines], axis=0)
        table = to_all(jnp.broadcast_to(table, (chips, *table.shape)), XY)
        return kernel_call(
            functools.partial(all_ancestors_body, sizes, sep, held), mail, 1024, 2 * MIB
        )(listed, table)

    ancestors = lax.cond(fits[0] == 1, few_ancestors, all_ancestors, blocks, value, lines, listed)

    own_rows, sent, leaf_rhs, leaf_update = kernel_call(
        ancestors_body,
        (
            array(n_leaf, wide),
            array(n_leaf + own_sep, wide),
            array(*leaf_rhs.shape),
            array(*leaf_update.shape),
        ),
        2 * cores * n_leaf * wide * chips * SLOTS,
        MIB,
        (0,),
        16,
        in_hbm=(4, 5),
        scratch=(pltpu.SemaphoreType.DMA((2,)),),
    )(core, place, ancestors, value, leaf_rhs, leaf_update)
    arrived = swapped(sent)
    leaf_out, sep_out = kernel_call(
        leaf_body,
        (array(*leaf_rhs.shape), array(own_sep, nrhs)),
        2 * nrhs * (leaf_inv.size + leaf_update.size),
        4 * MIB,
        (0, 1),
        out_hbm=(0,),
        scratch=(pltpu.VMEM(leaf_rhs.shape, BF16), pltpu.SemaphoreType.DMA((4,))),
    )(core, leaf_cols, own_rows, arrived, value, leaf_rhs, leaf_update, leaf_inv)
    return (sep_out, leaf_out)


def solution(mesh):
    finer = Mesh(mesh.devices.reshape(mesh.shape["grp"], 2, 2, 2, 2, 2), ALL)
    split = P(ALL, None)
    in_specs = (split, split, split, P("grp", None), split, split, split, split, P(ALL), split)
    return jax.shard_map(
        on_device, mesh=finer, in_specs=in_specs, out_specs=(split, split), check_vma=False
    )
```

```python
import functools

import jax
import jax.numpy as jnp
from jax import lax
from jax.experimental import pallas as pl
from jax.experimental.pallas import tpu as pltpu
from jax.sharding import Mesh
from jax.sharding import PartitionSpec as P

ALL = ("grp", "x_1", "x_0", "y_1", "y_0", "core")
XY = ("x_1", "x_0", "y_1", "y_0")
MIXED = ("y_0", "x_0", "y_1", "x_1")
SLOTS, LIST = 64, 8
BASE = 64
CORE = "core"
BF16, F32, I32 = jnp.bfloat16, jnp.float32, jnp.int32
MIB = 1 << 20


def to_all(blocks, axes):
    return lax.all_to_all(blocks, axes, 0, 0, tiled=True)


def swapped(value):
    return lax.ppermute(value, CORE, [(0, 1), (1, 0)])


def dot(a, b, dims=((1,), (0,))):
    return lax.dot_general(a, b, (dims, ((), ())), preferred_element_type=F32)


def column(row):
    size = 128
    eye = lax.broadcasted_iota(I32, (size, size), 0) == lax.broadcasted_iota(I32, (size, size), 1)
    parts = [
        jnp.sum(jnp.where(eye, row[:, i : i + size], F32(0.0)), axis=1, keepdims=True)
        for i in range(0, row.shape[1], size)
    ]
    return jnp.concatenate(parts, axis=0)


def chosen(places, lines):
    if places.shape[0] == 1:
        places = column(places.astype(F32)).astype(I32)
    at = lax.broadcasted_iota(I32, (places.shape[0], lines), 1)
    return jnp.where(at == places, F32(1.0), F32(0.0)).astype(BF16)


def kernel_call(body, outs, flops, n_bytes, in_smem=(), limit=16, in_hbm=(), out_hbm=(), scratch=()):
    def call(*args):
        specs = [
            pl.BlockSpec(
                memory_space=pltpu.SMEM if i in in_smem else pltpu.HBM if i in in_hbm else pltpu.VMEM
            )
            for i in range(len(args))
        ]
        return pl.pallas_call(
            body,
            out_shape=outs,
            in_specs=specs,
            out_specs=jax.tree.unflatten(
                jax.tree.structure(outs),
                [
                    pl.BlockSpec(
                        memory_space=pltpu.SMEM
                        if out.ndim == 1
                        else pltpu.HBM
                        if i in out_hbm
                        else pltpu.VMEM
                    )
                    for i, out in enumerate(jax.tree.leaves(outs))
                ],
            ),
            scratch_shapes=scratch,
            cost_estimate=pl.CostEstimate(flops=flops, bytes_accessed=n_bytes, transcendentals=0),
            compiler_params=pltpu.CompilerParams(vmem_limit_bytes=int(limit * MIB)),
        )(*args)

    return call


def log2(size):
    assert size & (size - 1) == 0
    return size.bit_length() - 1


def spot(chip):
    bits = [(chip >> i) & 1 for i in range(4)]
    return (bits[0] << 3) + (bits[2] << 2) + (bits[1] << 1) + bits[3]


def root_owner(rows, own, cores, devices, groups):
    device = (rows >> log2(own)) & (devices - 1)
    group = rows >> log2(own * devices)
    line = (group << log2(cores)) + (device & (cores - 1))
    return device >> log2(cores), (line << log2(own)) + (rows & (own - 1))


def ancestor_owner(sizes, sep, held, rows):
    chip, line = root_owner(rows - sep, *sizes)
    here = rows < sep
    return jnp.where(here, rows >> log2(held), chip), jnp.where(here, rows & (held - 1), held + line)


def before(size):
    lines = lax.broadcasted_iota(I32, (size, size), 0)
    return one(lines < lax.broadcasted_iota(I32, (size, size), 1))


def one(mask):
    return jnp.where(mask, F32(1.0), F32(0.0)).astype(BF16)


def encoded(rows):
    digits = [rows >> log2(BASE), rows & (BASE - 1)]
    size = 128
    lines = [d[:, i : i + size] for d in digits for i in range(0, rows.shape[1], size)]
    return jnp.concatenate(lines, axis=0).astype(F32).astype(BF16)


def decoded(lines):
    value = lines.astype(F32)
    half = value.shape[0] // 2
    value = value[:half] * F32(BASE) + value[half:]
    return jnp.concatenate([value[i : i + 1] for i in range(half)], axis=1).astype(I32)


def side(first, value):
    half = value.shape[1] // 2
    return jnp.where(first, value[:, :half], value[:, half:])


def of_core(first, value):
    half = value.shape[0] // 2
    return jnp.where(first, value[:half], value[half:])


def joined(first, mine, theirs):
    return jnp.concatenate(
        [jnp.where(first, mine, theirs), jnp.where(first, theirs, mine)], axis=1
    )


def fan_body(root, out):
    half = root.shape[1] // 2
    low, high = root[:, :half], root[:, half:]
    for i in range(0, out.shape[0], 2):
        out[i] = low
        out[i + 1] = high


def pack_body(
    core, rhs_at, update_at, rows_at, leaf_rows_at, out, kept, rhs, update, wanted, listed, sems
):
    pairs = ((rhs_at, rhs), (update_at, update), (rows_at, wanted), (leaf_rows_at, listed))
    fetches = [pltpu.make_async_copy(*pair, sems.at[i]) for i, pair in enumerate(pairs)]
    for fetch in fetches:
        fetch.start()
    for fetch in fetches:
        fetch.wait()
    rows, half = rhs.shape[0], rhs.shape[1] // 2
    first = core[0] == 0
    width = update.shape[1]
    leaf, sep = listed[...], wanted[...]
    digits = [
        jnp.concatenate([leaf >> log2(BASE), leaf & (BASE - 1)], axis=1),
        sep >> log2(BASE),
        sep & (BASE - 1),
    ]
    digits = jnp.concatenate(digits + [jnp.zeros((LIST - 3, width), I32)], axis=0)
    digits = digits.astype(F32).astype(BF16)
    for target, take in ((out, jnp.logical_not(first)), (kept, first)):
        target[:rows, :half] = side(take, rhs[...])
        target[:rows, half:] = update[...]
        target[rows:, :half] = jnp.zeros((LIST, half), BF16)
        target[rows:, half:] = digits


def plan_body(
    sizes, chip_at, kept, arrived, rhs_out, spread_out, select_out, list_out, fits_out
):
    own, half = kept.shape[0] - LIST, rhs_out.shape[1]
    chip = chip_at[0]
    rhs_out[...] = jnp.concatenate([kept[:own, :half], arrived[:own, :half]], axis=0)
    both = jnp.concatenate([kept[:own, half:], arrived[:own, half:]], axis=0)
    digits, other_digits = kept[own:, half:].astype(F32), arrived[own:, half:].astype(F32)

    chips = spread_out.shape[1] // SLOTS
    wanted = (digits[1:2] * F32(BASE) + digits[2:3]).astype(I32)
    size = wanted.shape[1]
    owner, line = root_owner(wanted, *sizes)
    owned = lax.broadcasted_iota(I32, (chips, size), 0) == owner
    rank = jnp.where(owned, dot(one(owned), before(size)), F32(0.0))
    rank = jnp.sum(rank, axis=0, keepdims=True).astype(I32)
    most = jnp.max(rank.astype(F32))
    fits = (most < F32(SLOTS)).astype(I32)
    fits_out[0] = fits
    place = jnp.where(fits == 1, owner * SLOTS + rank, lax.broadcasted_iota(I32, (1, size), 1))
    spread_out[...] = dot(both, chosen(place, spread_out.shape[1])).astype(BF16)

    mine = jnp.where(owner == chip, rank, -1)
    slot = one(lax.broadcasted_iota(I32, (SLOTS, size), 0) == mine)
    lines = select_out.shape[1]
    source = one(lax.broadcasted_iota(I32, (lines, size), 0) == line)
    select_out[...] = dot(slot, source, ((1,), (1,))).astype(BF16)

    listed = []
    for line in (digits[:1], other_digits[:1]):
        n_leaf = line.shape[1] // 2
        listed.append((line[:, :n_leaf] * F32(BASE) + line[:, n_leaf:]).astype(I32))
    list_out[...] = encoded(jnp.concatenate(listed, axis=1))


def select_body(select, lines, listed, out):
    rows = dot(select[...], lines[...]).astype(BF16)
    listed = listed[...]
    for i in range(out.shape[0]):
        out[i, :SLOTS] = rows
        out[i, SLOTS:] = listed


def all_lines_body(lines, listed, out):
    held = lines.shape[0]
    for i in range(out.shape[0]):
        out[i, :held] = lines[...]
        out[i, held:] = listed[...]


def all_rows_body(sizes, rows, arrived, out):
    chips, held, wide = arrived.shape
    held = held - LIST
    owner, line = root_owner(rows[...], *sizes)
    table = arrived[:, :held].reshape(chips * held, wide)
    picked = dot(chosen(owner * held + line, chips * held), table).astype(BF16)
    full = picked.shape[0] // SLOTS
    out[:full, :SLOTS] = picked.reshape(full, SLOTS, wide)
    if chips > full:
        out[full:, :SLOTS] = jnp.zeros((chips - full, SLOTS, wide), BF16)
    out[:, SLOTS:] = arrived[:, held:]


def terms_body(rhs, spread, arrived, own_inverse_at, other_inverse_at, out, own_inverse, other_inverse, sems):
    copies = (
        pltpu.make_async_copy(own_inverse_at, own_inverse, sems.at[0]),
        pltpu.make_async_copy(other_inverse_at, other_inverse, sems.at[1]),
    )
    for copy in copies:
        copy.start()
    chips, _, width = out.shape
    wide = rhs.shape[1]
    table = arrived[:, :SLOTS].reshape(chips * SLOTS, wide)
    residual = rhs[...].astype(F32) - dot(spread[...], table)
    residual = residual.astype(BF16).astype(F32).T.astype(BF16)
    for copy in copies:
        copy.wait()
    for i in range(chips):
        at = slice(i * width, (i + 1) * width)
        both = jnp.concatenate([own_inverse[:, at], other_inverse[:, at]], axis=0)
        out[spot(i)] = dot(residual, both).astype(BF16)


def leaf_plan_body(sizes, sep, held, chip_at, arrived, select_out, place_out, fits_out, mine_at, line_at):
    chips = arrived.shape[0]
    chip = chip_at[0]
    rows = jnp.concatenate([decoded(arrived[i, SLOTS:]) for i in range(chips)], axis=0)
    size = rows.shape[1]
    owner, line = ancestor_owner(sizes, sep, held, rows)
    counts = before(size)
    owned = jnp.concatenate([owner == i for i in range(chips)], axis=0)
    rank = jnp.where(owned, dot(one(owned), counts), F32(0.0))
    fits = (jnp.max(rank) < F32(SLOTS)).astype(I32)
    fits_out[0] = fits

    listed = lax.broadcasted_iota(I32, (chips, 1), 0) == chip
    own_rank = jnp.zeros((1, size), F32)
    for i in range(chips):
        part = rank[i * chips : (i + 1) * chips]
        own_rank = own_rank + jnp.sum(jnp.where(listed, part, F32(0.0)), axis=0, keepdims=True)
    own_owner = jnp.sum(jnp.where(listed, owner.astype(F32), F32(0.0)), axis=0, keepdims=True)
    place = own_owner * F32(SLOTS) + own_rank
    place = jnp.where(fits == 1, place, lax.broadcasted_iota(I32, (1, size), 1).astype(F32))
    place_out[...] = place.astype(I32)

    mine = owner == chip
    mine_at[...] = jnp.where(mine, dot(one(mine), counts), F32(-1.0)).astype(I32)
    line_at[...] = line

    def step(i, _):
        slot = one(lax.broadcasted_iota(I32, (SLOTS, size), 0) == mine_at[pl.ds(i, 1), :])
        lines = select_out.shape[2]
        source = one(lax.broadcasted_iota(I32, (lines, size), 0) == line_at[pl.ds(i, 1), :])
        select_out[i] = dot(slot, source, ((1,), (1,))).astype(BF16)
        return 0

    lax.fori_loop(0, chips, step, 0)


def sum_body(terms, select, lines, out, blocks):
    total = terms[0].astype(F32)
    for i in range(1, terms.shape[0]):
        total = total + terms[i].astype(F32)
    value = total.T.astype(BF16)
    out[...] = value
    table = jnp.concatenate([value, lines[...]], axis=0)
    chips, slots, size = select.shape
    rows = dot(select[...].reshape(chips * slots, size), table).astype(BF16)
    blocks[...] = rows.reshape(blocks.shape)


def all_ancestors_body(sizes, sep, held, listed, arrived, out):
    chips, lines, wide = arrived.shape
    owner, line = ancestor_owner(sizes, sep, held, decoded(listed[...]))
    place = owner * lines + line
    total = jnp.zeros((place.shape[1], wide), F32)
    for i in range(chips):
        total = total + dot(chosen(place - i * lines, lines), arrived[i])
    full = total.shape[0] // SLOTS
    out[:full] = total.astype(BF16).reshape(full, SLOTS, wide)
    if chips > full:
        out[full:] = jnp.zeros((chips - full, SLOTS, wide), BF16)


def ancestors_body(core, place, arrived, value, rhs_at, update_at, own, sent, rhs, update, sems):
    fetches = [
        pltpu.make_async_copy(update_at, update, sems.at[0]),
        pltpu.make_async_copy(rhs_at, rhs, sems.at[1]),
    ]
    for fetch in fetches:
        fetch.start()
    chips, slots, wide = arrived.shape
    table = arrived[...].reshape(chips * slots, wide)
    rows = dot(chosen(place[...], chips * slots), table).astype(BF16)
    half = rows.shape[0] // 2
    own[...] = rows[:half]
    sent[:half] = rows[half:]
    sent[half:] = of_core(core[0] != 0, value[...])
    for fetch in fetches:
        fetch.wait()


def leaf_body(core, cols, own, arrived, value, rhs, update, inverse, out, sep_out, block, sems):
    first, half = core[0] == 0, own.shape[0]
    rows = joined(first, own[...], arrived[:half])
    live = lax.broadcasted_iota(I32, out.shape, 0) < cols[0]
    residual = rhs[...].astype(F32) - dot(update[...], rows)
    residual = jnp.where(live, residual, F32(0.0)).astype(BF16)
    size = out.shape[0] // sems.shape[0]
    sent = []
    for i in range(sems.shape[0]):
        at = pl.ds(i * size, size)
        solved = dot(inverse[at, :], residual)
        live = lax.broadcasted_iota(I32, solved.shape, 0) < cols[0] - i * size
        block[at, :] = jnp.where(live, solved, F32(0.0)).astype(BF16)
        sent.append(pltpu.make_async_copy(block.at[at], out.at[at], sems.at[i]))
        sent[-1].start()
    sep_out[...] = joined(first, of_core(first, value[...]), arrived[half:])
    for copy in sent:
        copy.wait()


def on_device(
    root_solution,
    sep_rhs,
    sep_update,
    sep_rows,
    sep_inv_cols,
    leaf_rhs,
    leaf_update,
    leaf_rows,
    leaf_cols,
    leaf_inv,
):
    groups = lax.axis_size("grp")
    chips = lax.axis_size(XY)
    cores = lax.axis_size(CORE)
    devices = chips * cores
    core, chip = lax.axis_index(CORE).astype(I32)[None], lax.axis_index(XY).astype(I32)[None]
    own_root, nrhs = root_solution.shape
    own_sep, sep = sep_inv_cols.shape
    wide = nrhs // cores
    n_sep, n_leaf = sep_rows.shape[1], leaf_rows.shape[1]
    held = cores * own_sep
    lines_here = groups * cores * own_root
    sizes = (own_root, cores, devices, groups)

    def array(*shape, dtype=BF16):
        return jax.ShapeDtypeStruct(shape, dtype)

    flag = array(1, dtype=I32)

    blocks = kernel_call(fan_body, array(groups * cores, own_root, wide), 1024, MIB, limit=4)(
        root_solution
    )
    lines = to_all(blocks, ("grp", CORE)).reshape(lines_here, wide)

    other_inverse = swapped(sep_inv_cols)
    assert n_sep == 2 * n_leaf
    sent, kept = kernel_call(
        pack_body,
        (array(own_sep + LIST, wide + n_sep), array(own_sep + LIST, wide + n_sep)),
        own_sep,
        MIB,
        (0,),
        63.25,
        in_hbm=(1, 2, 3, 4),
        scratch=(
            pltpu.VMEM(sep_rhs.shape, BF16),
            pltpu.VMEM(sep_update.shape, BF16),
            pltpu.VMEM(sep_rows.shape, I32),
            pltpu.VMEM(leaf_rows.shape, I32),
            pltpu.SemaphoreType.DMA((4,)),
        ),
    )(core, sep_rhs, sep_update, sep_rows, leaf_rows)
    arrived = swapped(sent)

    rhs, spread, select, listed, fits = kernel_call(
        functools.partial(plan_body, sizes),
        (
            array(held, wide),
            array(held, chips * SLOTS),
            array(SLOTS, lines_here),
            array(LIST, 128),
            flag,
        ),
        2 * held * n_sep * chips * SLOTS,
        MIB,
        (0,),
    )(chip, kept, arrived)

    mail = array(chips, SLOTS + LIST, wide)
    blocks = kernel_call(select_body, mail, SLOTS * lines_here * wide, MIB, limit=4)(
        select, lines, listed
    )

    def few_rows(blocks, lines, listed, sep_rows):
        return to_all(blocks, XY)

    def all_rows(blocks, lines, listed, sep_rows):
        full = array(chips, lines_here + LIST, wide)
        full = kernel_call(all_lines_body, full, 1024, 2 * MIB)(lines, listed)
        return kernel_call(
            functools.partial(all_rows_body, sizes), mail, 1024, 2 * MIB
        )(sep_rows, to_all(full, XY))

    root_rows = lax.cond(fits[0] == 1, few_rows, all_rows, blocks, lines, listed, sep_rows)

    terms = kernel_call(
        terms_body,
        array(chips, wide, sep // chips),
        2 * held * wide * (chips * SLOTS + sep),
        6 * MIB,
        in_hbm=(3, 4),
        scratch=(
            pltpu.VMEM(sep_inv_cols.shape, BF16),
            pltpu.VMEM(sep_inv_cols.shape, BF16),
            pltpu.SemaphoreType.DMA((2,)),
        ),
    )(rhs, spread, root_rows, sep_inv_cols, other_inverse)
    terms = to_all(terms, MIXED)

    select, place, fits = kernel_call(
        functools.partial(leaf_plan_body, sizes, sep, held),
        (
            array(chips, SLOTS, held + lines_here),
            array(1, cores * n_leaf, dtype=I32),
            flag,
        ),
        chips * 2**26,
        2 * MIB,
        (0,),
        scratch=(
            pltpu.VMEM((chips, cores * n_leaf), I32),
            pltpu.VMEM((chips, cores * n_leaf), I32),
        ),
    )(chip, root_rows)
    mail = array(chips, SLOTS, wide)
    value, blocks = kernel_call(
        sum_body, (array(held, wide), mail), 2 * chips * SLOTS * wide * (held + lines_here), 2 * MIB
    )(terms, select, lines)

    def few_ancestors(blocks, value, lines, listed):
        return to_all(blocks, XY)

    def all_ancestors(blocks, value, lines, listed):
        table = jnp.concatenate([value, lines], axis=0)
        table = to_all(jnp.broadcast_to(table, (chips, *table.shape)), XY)
        return kernel_call(
            functools.partial(all_ancestors_body, sizes, sep, held), mail, 1024, 2 * MIB
        )(listed, table)

    ancestors = lax.cond(fits[0] == 1, few_ancestors, all_ancestors, blocks, value, lines, listed)

    own_rows, sent, leaf_rhs, leaf_update = kernel_call(
        ancestors_body,
        (
            array(n_leaf, wide),
            array(n_leaf + own_sep, wide),
            array(*leaf_rhs.shape),
            array(*leaf_update.shape),
        ),
        2 * cores * n_leaf * wide * chips * SLOTS,
        MIB,
        (0,),
        16,
        in_hbm=(4, 5),
        scratch=(pltpu.SemaphoreType.DMA((2,)),),
    )(core, place, ancestors, value, leaf_rhs, leaf_update)
    arrived = swapped(sent)
    leaf_out, sep_out = kernel_call(
        leaf_body,
        (array(*leaf_rhs.shape), array(own_sep, nrhs)),
        2 * nrhs * (leaf_inv.size + leaf_update.size),
        4 * MIB,
        (0, 1),
        out_hbm=(0,),
        scratch=(pltpu.VMEM(leaf_rhs.shape, BF16), pltpu.SemaphoreType.DMA((4,))),
    )(core, leaf_cols, own_rows, arrived, value, leaf_rhs, leaf_update, leaf_inv)
    return (sep_out, leaf_out)


def solution(mesh):
    finer = Mesh(mesh.devices.reshape(mesh.shape["grp"], 2, 2, 2, 2, 2), ALL)
    split = P(ALL, None)
    in_specs = (split, split, split, P("grp", None), split, split, split, split, P(ALL), split)
    return jax.shard_map(
        on_device, mesh=finer, in_specs=in_specs, out_specs=(split, split), check_vma=False
    )
```
